128 devices in a mesh: row: 16 (over x, z_hi, core), col: 8 (over y, z_lo).
Axes of the slice: x: 4, y: 4, z: 4 (z_hi: 2, z_lo: 2; z = z_hi * 2 + z_lo), core: 2. Of those that a mesh axis runs over, the one named last changes fastest.
Arguments:
- velocity: float32 [3, 2, 128, 256, 256], P(None, None, 'row', 'col'), may hold values from -7.5 to 7.5
- accumulator: float32 [3, 2, 128, 256, 256], P(None, None, 'row', 'col'), may hold values from -6 to 6
- remesh_flag: int32 [128], P('row'), may hold values 0 or 1
- remesh_shift: int32 [128], P('row'), may hold values from -128 to 127
- viscosity: float32 [1], replicated, may hold values from 0.0003 to 0.0015
- shear: float32 [1], replicated, may hold values from 8 to 20
- clock: float32 [1], replicated, may hold values from 0 to 0.05
- step: float32 [1], replicated, may hold values from 0.004 to 0.01
Outputs:
- new_velocity: float32 [3, 2, 128, 256, 256], P(None, None, 'row', 'col')
- new_accumulator: float32 [3, 2, 128, 256, 256], P(None, None, 'row', 'col')
- spectra: float32 [2, 128], P(None, 'row')
The draws below stay inside these ranges and needn't reach their ends.
All inputs are finite; a program needn't handle non-finite values. No bound on the sum of `remesh_flag` on one device may be relied on, other than what follows from the above.
Results may differ from the reference program's by a relative error of at most 0.0001.
Values sent between devices are 32-bit elements; how exact they have to be, the bound alone decides.
A program may use at most 192 MiB of HBM per device.

```python
import math
import jax
import jax.numpy as jnp

NX = 256
NY = 256
NZ = 256
KX = 128


def draw_velocity(key, part):
    first_key = jax.random.fold_in(jax.random.fold_in(key, 11), 0)
    sample = jnp.clip(jax.random.normal(first_key, (3, 2, KX, NZ, NY), jnp.float32), -4.0, 4.0)
    correlated = sample.at[1].add(-0.6 * sample[0])
    return correlated


def set_ends(entries, stream_key, smallest, top_value):
    shape = entries.shape
    spot = [jax.random.randint(jax.random.fold_in(stream_key, axis), (), 0, shape[axis]) for axis in range(len(shape))]
    entries = entries.at[tuple(spot)].set(smallest)
    longest = shape.index(max(shape))
    spot[longest] = (spot[longest] + 1) % shape[longest]
    return entries.at[tuple(spot)].set(top_value)


def block_levels(stream_key, extent, cuts, low, high):
    gain = 1.0
    for position, parts in cuts:
        heights = jax.random.uniform(jax.random.fold_in(jax.random.fold_in(stream_key, 6), position), (parts,), jnp.float32, low / len(cuts), high / len(cuts))
        gain = gain * jnp.repeat(jnp.exp(heights), extent[position] // parts).reshape((-1,) + (1,) * (len(extent) - 1 - position))
    return gain


def gaussian(key, shape, width, bound, cuts=(), held_as=jnp.bfloat16):
    values = width * jax.random.normal(key, shape, jnp.float32)
    if cuts:
        values = values * block_levels(key, shape, cuts, -0.22, 0.18)
    return jnp.clip(values, -bound, bound).astype(held_as)


def setup_inputs(seed: int = 0) -> dict:
    key_list = jax.random.split(jax.random.key(seed), 9)
    return {
        "velocity": draw_velocity(jax.random.fold_in(key_list[8], 71), 0),
        "accumulator": gaussian(key_list[1], (3, 2, KX, NZ, NY), 1.0, 6.0, ((2, 16), (3, 8)), jnp.float32),
        "remesh_flag": set_ends((jax.random.randint(key_list[2], (KX,), 0, 2) < 1).astype(jnp.int32), jax.random.fold_in(key_list[2], 1), 0, 1),
        "remesh_shift": set_ends(jax.random.randint(key_list[3], (KX,), 0 - NY // 2, NY // 2), jax.random.fold_in(key_list[3], 1), 0 - NY // 2, (NY // 2) - 1).astype(jnp.int32),
        "viscosity": jnp.clip(jnp.exp(jax.random.uniform(key_list[4], (1,), jnp.float32, math.log(0.0003), math.log(0.0015))), 0.0003, 0.0015),
        "shear": jnp.clip(jax.random.uniform(key_list[5], (1,), jnp.float32, 8.0, 20.0), 8.0, 20.0),
        "clock": jnp.clip(jax.random.uniform(key_list[6], (1,), jnp.float32, 0.0, 0.05), 0.0, 0.05),
        "step": jnp.clip(jax.random.uniform(key_list[7], (1,), jnp.float32, 0.004, 0.01), 0.004, 0.01),
    }


def signed_index(positions, period):
    return jnp.where(2 * positions < period, positions, positions - period)


def roll_rows(field, amounts):
    def shift_row(row_data, amount_one):
        return jnp.roll(row_data, -amount_one, axis=-1)
    return jax.vmap(shift_row, in_axes=(2, 0), out_axes=2)(field, amounts)


def project(real_part, imag_part, wave_vector, inverse_square):
    along_real = (wave_vector[0] * real_part[0] + wave_vector[1] * real_part[1] + wave_vector[2] * real_part[2]) * inverse_square
    along_imag = (wave_vector[0] * imag_part[0] + wave_vector[1] * imag_part[1] + wave_vector[2] * imag_part[2]) * inverse_square
    return (jnp.stack([real_part[number] - wave_vector[number] * along_real for number in range(3)]),
            jnp.stack([imag_part[number] - wave_vector[number] * along_imag for number in range(3)]))


def cross_product(first_one, second_one):
    return jnp.stack([first_one[1] * second_one[2] - first_one[2] * second_one[1],
                      first_one[2] * second_one[0] - first_one[0] * second_one[2],
                      first_one[0] * second_one[1] - first_one[1] * second_one[0]])


def to_grid(real_part, imag_part):
    weights = jnp.where(jnp.arange(KX) == 0, 1.0, 2.0).astype(jnp.float32)[:, None, None]
    result_list = []
    for number in range(3):
        half = weights * (real_part[number] + 1j * imag_part[number])
        full = jnp.zeros((NX, NZ, NY), half.dtype).at[:KX].set(half)
        result_list.append(jnp.real(jnp.fft.ifftn(full, norm="ortho")))
    return jnp.stack(result_list)


def reference(velocity, accumulator, remesh_flag, remesh_shift, viscosity, shear, clock, step):
    offset = remesh_flag * remesh_shift
    remeshed = roll_rows(velocity, offset)
    carried = roll_rows(accumulator, offset)
    lattice_x = jnp.arange(KX, dtype=jnp.int32)
    lattice_z = signed_index(jnp.arange(NZ, dtype=jnp.int32), NZ)
    lattice_y = signed_index(jnp.arange(NY, dtype=jnp.int32), NY)
    wave_x = lattice_x.astype(jnp.float32)[:, None, None]
    wave_z = lattice_z.astype(jnp.float32)[None, :, None]
    wave_y = lattice_y.astype(jnp.float32)[None, None, :] - shear[0] * clock[0] * wave_x
    wave_vector = (wave_x, wave_y, wave_z)
    square_wave = wave_x * wave_x + wave_y * wave_y + wave_z * wave_z
    inverse_square = 1.0 / jnp.maximum(square_wave, 1.0)
    dealias_mask = ((3 * lattice_x < NX)[:, None, None] & (3 * jnp.abs(lattice_z) < NZ)[None, :, None]
                    & (3 * jnp.abs(lattice_y) < NY)[None, None, :]).astype(jnp.float32)
    solen_real, solen_imag = project(remeshed[:, 0], remeshed[:, 1], wave_vector, inverse_square)
    smooth_real = dealias_mask * solen_real
    smooth_imag = dealias_mask * solen_imag
    vort_real = -cross_product(wave_vector, smooth_imag)
    vort_imag = cross_product(wave_vector, smooth_real)
    flow_grid = to_grid(smooth_real, smooth_imag)
    swirl_grid = to_grid(vort_real, vort_imag)
    lamb_grid = cross_product(flow_grid, swirl_grid)
    lamb_hat = [jnp.fft.fftn(lamb_grid[number], norm="ortho")[:KX] for number in range(3)]
    hat_real = dealias_mask * jnp.stack([jnp.real(spectrum) for spectrum in lamb_hat])
    hat_imag = dealias_mask * jnp.stack([jnp.imag(spectrum) for spectrum in lamb_hat])
    proj_real, proj_imag = project(hat_real, hat_imag, wave_vector, inverse_square)
    shear_rate = shear[0]
    viscous_rate = viscosity[0]
    coupling = 2.0 * shear_rate * wave_x * inverse_square

    def tendency(projected, state):
        term_list = [projected[number] + coupling * wave_vector[number] * state[1] - viscous_rate * square_wave * state[number] for number in range(3)]
        term_list[0] = term_list[0] - shear_rate * state[1]
        return jnp.stack(term_list)

    tendencies = jnp.stack([tendency(proj_real, remeshed[:, 0]), tendency(proj_imag, remeshed[:, 1])], axis=1)
    new_accumulator = (-5.0 / 9.0) * carried + step[0] * tendencies
    new_velocity = remeshed + (15.0 / 16.0) * new_accumulator
    stress = jnp.sum(remeshed[0, 0] * remeshed[1, 0] + remeshed[0, 1] * remeshed[1, 1], axis=(1, 2)) / (NY * NZ)
    energy = jnp.sum(remeshed * remeshed, axis=(0, 1))
    dissipation = 2.0 * viscous_rate * jnp.sum(square_wave * energy, axis=(1, 2)) / (NY * NZ)
    return new_velocity, new_accumulator, jnp.stack([stress, dissipation])
```

```python
import numpy as np
import jax
import jax.numpy as jnp
from jax import lax
from jax.experimental import pallas as pl
from jax.experimental.pallas import tpu as pltpu
from jax.sharding import PartitionSpec as P

N = 256
ROWS = 11
F32 = jnp.float32
BF16 = jnp.bfloat16
VLIM = 60 * 1024 * 1024


def halves(table):
    table = table.astype(np.float32)
    high = table.astype(jnp.bfloat16)
    low = (table - high.astype(np.float32)).astype(jnp.bfloat16)
    return np.stack([high, low])


def tables():
    index = np.arange(N)
    angle = (index[:, None] * index[None, :] % N) * (2.0 * np.pi / N)
    cos, sin = np.cos(angle) / 16.0, np.sin(angle) / 16.0
    first = np.block([[cos, -sin], [sin, cos]])
    second = np.block([[cos, sin], [-sin, cos]])
    count = ROWS * 8
    weights = np.where(np.arange(count) == 0, 1.0, 2.0)
    back_x = np.concatenate([cos[:, :count] * weights, -sin[:, :count] * weights], axis=1)
    fore_x = np.concatenate([cos[:count], -sin[:count]], axis=0)
    return halves(first), halves(second), halves(back_x), halves(fore_x)


def split(value):
    high = value.astype(BF16)
    return high, (value - high.astype(F32)).astype(BF16)


def dot3(left, right, dims=((1,), (0,))):
    def one(a, b):
        return lax.dot_general(a, b, (dims, ((), ())), preferred_element_type=F32)

    return one(left[0], right[0]) + one(left[1], right[0]) + one(left[0], right[1])


def swap_chunks(items, width):
    items = list(items)
    count = len(items)
    lane = lax.broadcasted_iota(jnp.int32, items[0].shape, items[0].ndim - 1) // width
    axis = items[0].ndim - 1
    step = count // 2
    while step:
        keep = (lane & step) == 0
        for i in range(count):
            if i & step == 0:
                a, b = items[i], items[i + step]
                items[i] = jnp.where(keep, a, pltpu.roll(b, step * width, axis))
                items[i + step] = jnp.where(keep, pltpu.roll(a, 128 - step * width, axis), b)
        step //= 2
    return items


def swap_wide(items):
    out = [[None, None] for _ in range(8)]
    for g in range(2):
        for h in range(2):
            part = swap_chunks([items[4 * g + i][:, 128 * h:128 * h + 128] for i in range(4)], 32)
            for j in range(4):
                out[4 * h + j][g] = part[j]
    return [jnp.concatenate(pair, axis=1) for pair in out]


def signed(index):
    return jnp.where(2 * index < N, index, index - N)


def modes(kx_index, kz_index, ky_index, drift):
    wave_x = kx_index.astype(F32)
    wave_z = signed(kz_index).astype(F32)
    wave_y = signed(ky_index).astype(F32) - drift * wave_x
    square = wave_x * wave_x + wave_y * wave_y + wave_z * wave_z
    mask = (3 * kx_index < N) & (3 * jnp.abs(signed(kz_index)) < N) & (3 * jnp.abs(signed(ky_index)) < N)
    return wave_x, wave_y, wave_z, square, mask


def joined(data):
    return jnp.concatenate([data[g] for g in range(4)], axis=1)


def pre_kernel(place, offset, scal, velocity, high_out, low_out, sums_out):
    step = pl.program_id(0)
    shift = (0 - offset[step]) & (N - 1)
    kx = jnp.full((32, N), place[0] * 8 + step, jnp.int32)
    kz = lax.broadcasted_iota(jnp.int32, (32, N), 0) + place[1] * 32
    ky = lax.broadcasted_iota(jnp.int32, (32, N), 1)
    wave_x, wave_y, wave_z, square, mask = modes(kx, kz, ky, scal[1] * scal[2])
    inverse = 1.0 / jnp.maximum(square, 1.0)
    wave = (wave_x, wave_y, wave_z)
    energy = jnp.zeros((32, N), F32)
    stress = jnp.zeros((32, N), F32)
    for p in range(2):
        v = [pltpu.roll(velocity[c, p, 0], shift, 1) for c in range(3)]
        energy += v[0] * v[0] + v[1] * v[1] + v[2] * v[2]
        stress += v[0] * v[1]
        along = (wave[0] * v[0] + wave[1] * v[1] + wave[2] * v[2]) * inverse
        for c in range(3):
            high, low = split(jnp.where(mask, v[c] - wave[c] * along, 0.0))
            high_out[c, :, p * N:(p + 1) * N] = high
            low_out[c, :, p * N:(p + 1) * N] = low
    def total(value):
        value = jnp.sum(value, axis=0, keepdims=True)
        return value[:, :128] + value[:, 128:]
    sums_out[0, 0:1, :] = total(stress)
    sums_out[0, 1:2, :] = total(square * energy)


def y_back(high, low, first, out):
    result = dot3((first[0], first[1]), (high[0], low[0]), ((1,), (1,)))
    for c in range(8):
        for p in range(2):
            out[c, 0, p] = result[p * N + 32 * c:p * N + 32 * c + 32]


def z_back(block, second, out, data):
    for p in range(2):
        moved = swap_wide([block[s, 0, p] for s in range(8)])
        for kx in range(8):
            for g in range(2):
                data[2 * p + g, pl.ds(kx, 32, stride=8), :] = moved[kx][:, 128 * g:128 * g + 128]
    result = dot3(split(joined(data)), (second[0], second[1])).reshape(4, 8, 8, 2 * N)
    for p in range(2):
        for h in range(2):
            lanes = slice(p * N + 128 * h, p * N + 128 * h + 128)
            moved = swap_chunks([result[:, i, :, lanes] for i in range(8)], 16)
            for r in range(8):
                for j in range(4):
                    out[8 * h + r, 0, p, :, 128 * j:128 * j + 128] = moved[r][j]


def x_both(block, back, fore, out):
    lanes = block.shape[-1]
    count = ROWS * 8
    u = []
    for c in range(3):
        both = jnp.concatenate([block[:ROWS, c, p].reshape(count, lanes) for p in range(2)], axis=0)
        u.append(dot3((back[0], back[1]), split(both)))
    square = u[0] * u[0]
    fields = [u[0] * u[1], u[0] * u[2], u[1] * u[2], u[1] * u[1] - square, u[2] * u[2] - square]
    for t in range(5):
        hat = dot3((fore[0], fore[1]), split(fields[t])).reshape(2, ROWS, 8, lanes)
        for p in range(2):
            for r in range(ROWS):
                out[r, t, p] = hat[p, r]
            for r in range(ROWS, 16):
                out[r, t, p] = jnp.zeros((8, lanes), F32)


def z_fore(place, block, first, out, data, hats):
    for t in range(5):
        for p in range(2):
            for h in range(2):
                for j in range(4):
                    moved = swap_chunks([block[8 * h + s, t, p, :, 128 * j:128 * j + 128] for s in range(8)], 16)
                    for i in range(8):
                        data[2 * p + h, (8 * j + i) * 8:(8 * j + i) * 8 + 8, :] = moved[i]
        hats[t] = dot3(split(joined(data)), (first[0], first[1]))
    kx_index = (lax.broadcasted_iota(jnp.int32, (N, N), 0) & 7) + place[0] * 8
    kz_index = lax.broadcasted_iota(jnp.int32, (N, N), 1)
    kx = kx_index.astype(F32)
    kz = signed(kz_index).astype(F32)
    origin = (kx_index == 0) & (kz_index == 0)
    for p in range(2):
        t01, t02, t12, t11, t22 = [hats[t, :, p * N:(p + 1) * N] for t in range(5)]
        cross = kx * kz
        fields = [
            jnp.where(origin, t01, kx * t01 + kz * t12),
            2.0 * cross * t02 + kz * kz * t22 - (kx * kx + kz * kz) * t11,
            (kz * kz - kx * kx) * t02 - cross * t22,
            jnp.where(origin, t12, kz * t01 - kx * t12),
        ]
        for g in range(4):
            for h in range(2):
                data[h] = fields[g][:, 128 * h:128 * h + 128]
            moved = swap_wide([jnp.concatenate([data[h, pl.ds(i, 32, stride=8), :] for h in range(2)], axis=1) for i in range(8)])
            for c in range(8):
                out[c, g, p] = moved[c]


def post_kernel(place, offset, scal, block, second, velocity, accumulator, new_velocity, new_accumulator):
    step = pl.program_id(0)
    drift = scal[1] * scal[2]
    hats = []
    for g in range(4):
        both = jnp.concatenate([block[:, g, p].reshape(N, 128) for p in range(2)], axis=0)
        result = dot3((second[0], second[1]), split(both))
        hats.append((result[:N], result[N:]))
    lane = lax.broadcasted_iota(jnp.int32, (N, 128), 1)
    kx_index = lane // 32 + (place[0] * 8 + step * 4)
    kz_index = lane % 32 + place[1] * 32
    ky_index = lax.broadcasted_iota(jnp.int32, (N, 128), 0)
    kx, k1, kz, square, mask = modes(kx_index, kz_index, ky_index, drift)
    flat = kx * kx + kz * kz
    origin = flat == 0.0
    over_square = 1.0 / jnp.maximum(square, 1.0)
    over_flat = 1.0 / jnp.maximum(flat, 1.0)
    result = [[None, None] for _ in range(3)]
    for p in range(2):
        sign = -1.0 if p == 0 else 1.0
        x, q, r, s = [sign * hats[g][1 - p] for g in range(4)]
        v = ((k1 * k1 - flat) * x + k1 * q) * over_square
        w = 0.0 - (r + k1 * s)
        part = [
            jnp.where(origin, 0.0 - k1 * x, (kz * w - kx * k1 * v) * over_flat),
            jnp.where(origin, 0.0, v),
            jnp.where(origin, 0.0 - k1 * s, (0.0 - kx * w - kz * k1 * v) * over_flat),
        ]
        for c in range(3):
            result[c][p] = jnp.where(mask, part[c], 0.0).T
    for i in range(4):
        shift = (0 - offset[step * 4 + i]) & (N - 1)
        kx_index = jnp.full((32, N), place[0] * 8 + step * 4 + i, jnp.int32)
        kz_index = lax.broadcasted_iota(jnp.int32, (32, N), 0) + place[1] * 32
        ky_index = lax.broadcasted_iota(jnp.int32, (32, N), 1)
        kx, k1, kz, square, _ = modes(kx_index, kz_index, ky_index, drift)
        wave = (kx, k1, kz)
        coupling = 2.0 * scal[1] * kx / jnp.maximum(square, 1.0)
        damp = scal[0] * square
        for p in range(2):
            v = [pltpu.roll(velocity[c, p, i], shift, 1) for c in range(3)]
            for c in range(3):
                rate = result[c][p][32 * i:32 * i + 32] + coupling * wave[c] * v[1] - damp * v[c]
                if c == 0:
                    rate = rate - scal[1] * v[1]
                fresh = (-5.0 / 9.0) * pltpu.roll(accumulator[c, p, i], shift, 1) + scal[3] * rate
                new_accumulator[c, p, i] = fresh
                new_velocity[c, p, i] = v[c] + (15.0 / 16.0) * fresh


def call(kernel, grid, ins, outs, scratch=()):
    return pl.pallas_call(
        kernel,
        grid=grid,
        in_specs=ins,
        out_specs=[spec for spec, _ in outs],
        out_shape=[shape for _, shape in outs],
        scratch_shapes=list(scratch),
        compiler_params=pltpu.CompilerParams(vmem_limit_bytes=VLIM),
    )


def spec(shape, index):
    return pl.BlockSpec(shape, index)


def whole(array):
    rank = array.ndim
    return pl.BlockSpec(array.shape, lambda *_: (0,) * rank)


SMEM = pl.BlockSpec(memory_space=pltpu.SMEM)


def exchange(value, axis):
    return lax.all_to_all(value, axis, split_axis=0, concat_axis=0, tiled=True)


def body(velocity, accumulator, remesh_flag, remesh_shift, viscosity, shear, clock, step):
    first, second, back, fore = [jnp.asarray(table) for table in tables()]
    place = jnp.stack([lax.axis_index("row"), lax.axis_index("col")]).astype(jnp.int32)
    offset = remesh_flag * remesh_shift
    scal = jnp.concatenate([viscosity, shear, clock, step])
    shape = jax.ShapeDtypeStruct
    high, low, sums = call(
        pre_kernel, (8,),
        [SMEM, SMEM, SMEM, spec((3, 2, 1, 32, N), lambda i: (0, 0, i, 0, 0))],
        [(spec((3, 32, 2 * N), lambda i: (0, i, 0)), shape((3, N, 2 * N), BF16)),
         (spec((3, 32, 2 * N), lambda i: (0, i, 0)), shape((3, N, 2 * N), BF16)),
         (spec((1, 8, 128), lambda i: (i, 0, 0)), shape((8, 8, 128), F32))],
    )(place, offset, scal, velocity)
    [one] = call(
        y_back, (3,),
        [spec((1, N, 2 * N), lambda f: (f, 0, 0)), spec((1, N, 2 * N), lambda f: (f, 0, 0)), whole(first)],
        [(spec((8, 1, 2, 32, N), lambda f: (0, f, 0, 0, 0)), shape((8, 3, 2, 32, N), F32))],
    )(high, low, first)
    one = exchange(one, "col")
    [two] = call(
        z_back, (3,),
        [spec((8, 1, 2, 32, N), lambda f: (0, f, 0, 0, 0)), whole(second)],
        [(spec((16, 1, 2, 8, 2 * N), lambda f: (0, f, 0, 0, 0)), shape((16, 3, 2, 8, 2 * N), F32))],
        [pltpu.VMEM((4, N, 128), F32)],
    )(one, second)
    two = exchange(two, "row")
    [three] = call(
        x_both, (2,),
        [spec((16, 3, 2, 8, N), lambda i: (0, 0, 0, 0, i)), whole(back), whole(fore)],
        [(spec((16, 5, 2, 8, N), lambda i: (0, 0, 0, 0, i)), shape((16, 5, 2, 8, 2 * N), F32))],
    )(two, back, fore)
    three = exchange(three, "row")
    [four] = call(
        z_fore, (1,),
        [SMEM, whole(three), whole(first)],
        [(spec((8, 4, 2, 32, N), lambda i: (0, 0, 0, 0, 0)), shape((8, 4, 2, 32, N), F32))],
        [pltpu.VMEM((4, N, 128), F32), pltpu.VMEM((5, N, 2 * N), F32)],
    )(place, three, first)
    four = exchange(four, "col")
    state = spec((3, 2, 4, 32, N), lambda i: (0, 0, i, 0, 0))
    new_velocity, new_accumulator = call(
        post_kernel, (2,),
        [SMEM, SMEM, SMEM, spec((8, 4, 2, 32, 128), lambda i: (0, 0, 0, 0, i)), whole(second), state, state],
        [(state, shape(velocity.shape, F32)), (state, shape(velocity.shape, F32))],
    )(place, offset, scal, four, second, velocity, accumulator)
    total = lax.psum(jnp.sum(sums[:, :2], axis=2), "col")
    scale = jnp.stack([jnp.ones((), F32), 2.0 * viscosity[0]]) / (N * N)
    return new_velocity, new_accumulator, total.T * scale[:, None]


def solution(mesh):
    state = P(None, None, "row", "col", None)
    return jax.shard_map(
        body,
        mesh=mesh,
        in_specs=(state, state, P("row"), P("row"), P(), P(), P(), P()),
        out_specs=(state, state, P(None, "row")),
        check_vma=False,
    )
```

```python
import numpy as np
import jax
import jax.numpy as jnp
from jax import lax
from jax.experimental import pallas as pl
from jax.experimental.pallas import tpu as pltpu
from jax.sharding import PartitionSpec as P

N = 256
ROWS = 11
F32 = jnp.float32
BF16 = jnp.bfloat16
VLIM = 60 * 1024 * 1024


def halves(table):
    table = table.astype(np.float32)
    high = table.astype(jnp.bfloat16)
    low = (table - high.astype(np.float32)).astype(jnp.bfloat16)
    return np.stack([high, low])


def tables():
    index = np.arange(N)
    angle = (index[:, None] * index[None, :] % N) * (2.0 * np.pi / N)
    cos, sin = np.cos(angle) / 16.0, np.sin(angle) / 16.0
    first = np.block([[cos, -sin], [sin, cos]])
    second = np.block([[cos, sin], [-sin, cos]])
    count = ROWS * 8
    weights = np.where(np.arange(count) == 0, 1.0, 2.0)
    back_x = np.concatenate([cos[:, :count] * weights, -sin[:, :count] * weights], axis=1)
    fore_x = np.concatenate([cos[:count], -sin[:count]], axis=0)
    return halves(first), halves(second), halves(back_x), halves(fore_x)


def split(value):
    high = value.astype(BF16)
    return high, (value - high.astype(F32)).astype(BF16)


def dot3(left, right, dims=((1,), (0,))):
    def one(a, b):
        return lax.dot_general(a, b, (dims, ((), ())), preferred_element_type=F32)

    return one(left[0], right[0]) + one(left[1], right[0]) + one(left[0], right[1])


def swap_chunks(items, width):
    items = list(items)
    count = len(items)
    lane = lax.broadcasted_iota(jnp.int32, items[0].shape, items[0].ndim - 1) // width
    axis = items[0].ndim - 1
    step = count // 2
    while step:
        keep = (lane & step) == 0
        for i in range(count):
            if i & step == 0:
                a, b = items[i], items[i + step]
                items[i] = jnp.where(keep, a, pltpu.roll(b, step * width, axis))
                items[i + step] = jnp.where(keep, pltpu.roll(a, 128 - step * width, axis), b)
        step //= 2
    return items


def swap_wide(items):
    out = [[None, None] for _ in range(8)]
    for g in range(2):
        for h in range(2):
            part = swap_chunks([items[4 * g + i][:, 128 * h:128 * h + 128] for i in range(4)], 32)
            for j in range(4):
                out[4 * h + j][g] = part[j]
    return [jnp.concatenate(pair, axis=1) for pair in out]


def signed(index):
    return jnp.where(2 * index < N, index, index - N)


def modes(kx_index, kz_index, ky_index, drift):
    wave_x = kx_index.astype(F32)
    wave_z = signed(kz_index).astype(F32)
    wave_y = signed(ky_index).astype(F32) - drift * wave_x
    square = wave_x * wave_x + wave_y * wave_y + wave_z * wave_z
    mask = (3 * kx_index < N) & (3 * jnp.abs(signed(kz_index)) < N) & (3 * jnp.abs(signed(ky_index)) < N)
    return wave_x, wave_y, wave_z, square, mask


def joined(data):
    return jnp.concatenate([data[g] for g in range(4)], axis=1)


def pre_kernel(place, offset, scal, velocity, high_out, low_out, sums_out):
    step = pl.program_id(0)
    shift = (0 - offset[step]) & (N - 1)
    kx = jnp.full((32, N), place[0] * 8 + step, jnp.int32)
    kz = lax.broadcasted_iota(jnp.int32, (32, N), 0) + place[1] * 32
    ky = lax.broadcasted_iota(jnp.int32, (32, N), 1)
    wave_x, wave_y, wave_z, square, mask = modes(kx, kz, ky, scal[1] * scal[2])
    inverse = 1.0 / jnp.maximum(square, 1.0)
    wave = (wave_x, wave_y, wave_z)
    energy = jnp.zeros((32, N), F32)
    stress = jnp.zeros((32, N), F32)
    for p in range(2):
        v = [pltpu.roll(velocity[c, p, 0], shift, 1) for c in range(3)]
        energy += v[0] * v[0] + v[1] * v[1] + v[2] * v[2]
        stress += v[0] * v[1]
        along = (wave[0] * v[0] + wave[1] * v[1] + wave[2] * v[2]) * inverse
        for c in range(3):
            high, low = split(jnp.where(mask, v[c] - wave[c] * along, 0.0))
            high_out[c, :, p * N:(p + 1) * N] = high
            low_out[c, :, p * N:(p + 1) * N] = low
    def total(value):
        value = jnp.sum(value, axis=0, keepdims=True)
        return value[:, :128] + value[:, 128:]
    sums_out[pl.ds(step, 1), :] = jnp.concatenate([total(stress), total(square * energy)], axis=1)


MESH = pl.DeviceIdType.MESH


def middle_kernel(high, low, sums, first, second, back, fore, hats_out, total_out,
                  send_c, recv_c, send_r, recv_r, send_rf, recv_rf, send_cf, recv_cf, recv_s,
                  u, hats, data, out_sems, in_sems):
    row, col = lax.axis_index("row"), lax.axis_index("col")
    row_on = row < ROWS
    col_on = (col != 3) & (col != 4)
    both_on = row_on & col_on

    def push(src, dst, sem, **device):
        return pltpu.make_async_remote_copy(
            src_ref=src, dst_ref=dst, send_sem=out_sems.at[sem], recv_sem=in_sems.at[sem],
            device_id=device, device_id_type=MESH)

    def drain(ref, sem):
        pltpu.make_async_copy(ref, ref, sem).wait()

    barrier = pltpu.get_barrier_semaphore()
    for i in range(1, 16):
        pl.semaphore_signal(barrier, inc=1, device_id={"row": (row + i) % 16}, device_id_type=MESH)
    for i in range(1, 8):
        pl.semaphore_signal(barrier, inc=1, device_id={"col": (col + i) % 8}, device_id_type=MESH)
    pl.semaphore_wait(barrier, 22)
    for i in range(1, 8):
        push(sums, recv_s.at[col], 15, col=(col + i) % 8).start()

    @pl.when(both_on)
    def _():
        def y_back(f, carry):
            result = dot3((first[0], first[1]), (high[f], low[f]), ((1,), (1,)))
            for c in range(8):
                for p in range(2):
                    send_c[f, c, p] = result[p * N + 32 * c:p * N + 32 * c + 32]
            for i in range(1, 8):
                to = (col + i) % 8
                push(send_c.at[f, to], recv_c.at[f, col], f, col=to).start()
            recv_c[f, col] = send_c[f, col]
            return carry

        lax.fori_loop(0, 3, y_back, 0)

    @pl.when(row_on)
    def _():
        def z_back(f, carry):
            @pl.when(col_on)
            def _():
                drain(recv_c.at[f, pl.ds(0, 5)], in_sems.at[f])

            @pl.when(jnp.logical_not(col_on))
            def _():
                drain(recv_c.at[f, pl.ds(0, 6)], in_sems.at[f])

            for p in range(2):
                blank = jnp.zeros((32, N), F32)
                moved = swap_wide([blank if s in (3, 4) else recv_c[f, s, p] for s in range(8)])
                for kx in range(8):
                    for g in range(2):
                        data[2 * p + g, pl.ds(kx, 32, stride=8), :] = moved[kx][:, 128 * g:128 * g + 128]
            result = dot3(split(joined(data)), (second[0], second[1])).reshape(4, 8, 8, 2 * N)
            for p in range(2):
                for h in range(2):
                    lanes = slice(p * N + 128 * h, p * N + 128 * h + 128)
                    moved = swap_chunks([result[:, i, :, lanes] for i in range(8)], 16)
                    for r in range(8):
                        for j in range(4):
                            send_r[f, 8 * h + r, p, :, 128 * j:128 * j + 128] = moved[r][j]
            for i in range(1, 16):
                to = (row + i) % 16
                push(send_r.at[f, to], recv_r.at[f, row], 3 + f, row=to).start()
            recv_r[f, row] = send_r[f, row]
            return carry

        lax.fori_loop(0, 3, z_back, 0)

    count = ROWS * 8

    def x_back(f, carry):
        @pl.when(row_on)
        def _():
            drain(recv_r.at[f, pl.ds(0, ROWS - 1)], in_sems.at[3 + f])

        @pl.when(jnp.logical_not(row_on))
        def _():
            drain(recv_r.at[f, pl.ds(0, ROWS)], in_sems.at[3 + f])

        for h in range(2):
            lanes = slice(N * h, N * h + N)
            both = jnp.concatenate([recv_r[f, :ROWS, p, :, lanes].reshape(count, N) for p in range(2)], axis=0)
            u[f, :, lanes] = dot3((back[0], back[1]), split(both))
        return carry

    lax.fori_loop(0, 3, x_back, 0)

    def x_fore(t, carry):
        a = jnp.where((t == 0) | (t == 2), 0, jnp.where(t == 3, 2, 1))
        b = jnp.where((t == 0) | (t == 4), 1, 2)
        weight = jnp.where(t >= 3, 1.0, 0.0)
        for h in range(2):
            lanes = slice(N * h, N * h + N)
            field = u[a, :, lanes] * u[b, :, lanes] - weight * (u[0, :, lanes] * u[0, :, lanes])
            hat = dot3((fore[0], fore[1]), split(field)).reshape(2, ROWS, 8, N)
            for p in range(2):
                for r in range(ROWS):
                    send_rf[t, r, p, :, lanes] = hat[p, r]
        for i in range(1, 16):
            to = (row + i) % 16

            @pl.when(to < ROWS)
            def _():
                push(send_rf.at[t, to], recv_rf.at[t, row], 6 + t, row=to).start()

        @pl.when(row_on)
        def _():
            recv_rf[t, row] = send_rf[t, row]

        return carry

    lax.fori_loop(0, 5, x_fore, 0)

    @pl.when(row_on)
    def _():
        def field_out(g, formula):
            for p in range(2):
                value = formula(p)
                for h in range(2):
                    data[h] = value[:, 128 * h:128 * h + 128]
                moved = swap_wide([jnp.concatenate([data[h, pl.ds(i, 32, stride=8), :] for h in range(2)], axis=1)
                                   for i in range(8)])
                for c in range(8):
                    if c not in (3, 4):
                        send_cf[g, c, p] = moved[c]
            for i in range(1, 8):
                to = (col + i) % 8

                @pl.when((to != 3) & (to != 4))
                def _():
                    push(send_cf.at[g, to], recv_cf.at[g, col], 11 + g, col=to).start()

            @pl.when(col_on)
            def _():
                recv_cf[g, col] = send_cf[g, col]

        def z_fore(t, carry):
            drain(recv_rf.at[t, pl.ds(0, 15)], in_sems.at[6 + t])
            for p in range(2):
                for h in range(2):
                    for j in range(4):
                        moved = swap_chunks([recv_rf[t, 8 * h + s, p, :, 128 * j:128 * j + 128] for s in range(8)], 16)
                        for i in range(8):
                            data[2 * p + h, (8 * j + i) * 8:(8 * j + i) * 8 + 8, :] = moved[i]
            hats[t] = dot3(split(joined(data)), (first[0], first[1]))

            kx_index = (lax.broadcasted_iota(jnp.int32, (N, N), 0) & 7) + row * 8
            kz_index = lax.broadcasted_iota(jnp.int32, (N, N), 1)
            kx = kx_index.astype(F32)
            kz = signed(kz_index).astype(F32)
            origin = (kx_index == 0) & (kz_index == 0)

            def part(number, p):
                return hats[number, :, p * N:(p + 1) * N]

            @pl.when(t == 1)
            def _():
                field_out(0, lambda p: jnp.where(origin, part(0, p), kx * part(0, p) + kz * part(1, p)))
                field_out(3, lambda p: jnp.where(origin, part(1, p), kz * part(0, p) - kx * part(1, p)))

            @pl.when(t == 3)
            def _():
                field_out(2, lambda p: (kz * kz - kx * kx) * part(2, p) - kx * kz * part(3, p))

            @pl.when(t == 4)
            def _():
                field_out(1, lambda p: 2.0 * kx * kz * part(2, p) + kz * kz * part(3, p) - (kx * kx + kz * kz) * part(4, p))

            return carry

        lax.fori_loop(0, 5, z_fore, 0)

    @pl.when(both_on)
    def _():
        def y_fore(step, carry):
            g = jnp.where(step == 0, 0, 4 - step)
            drain(recv_cf.at[g, pl.ds(0, 7)], in_sems.at[11 + g])
            both = jnp.concatenate([recv_cf[g, :, p].reshape(N, N) for p in range(2)], axis=0)
            hats_out[g] = dot3((second[0], second[1]), split(both))
            return carry

        lax.fori_loop(0, 4, y_fore, 0)

    @pl.when(jnp.logical_not(both_on))
    def _():
        for g in range(4):
            hats_out[g] = jnp.zeros((2 * N, N), F32)

    drain(recv_s.at[pl.ds(0, 7)], in_sems.at[15])
    recv_s[col] = sums[...]
    total = recv_s[0]
    for i in range(1, 8):
        total = total + recv_s[i]
    total_out[...] = total

    drain(recv_s.at[pl.ds(0, 7)], out_sems.at[15])

    @pl.when(both_on)
    def _():
        for f in range(3):
            drain(send_c.at[f, pl.ds(0, 7)], out_sems.at[f])

    @pl.when(row_on)
    def _():
        for f in range(3):
            drain(send_r.at[f, pl.ds(0, 15)], out_sems.at[3 + f])
        for t in range(5):
            drain(send_rf.at[t, pl.ds(0, ROWS - 1)], out_sems.at[6 + t])
        for g in range(4):
            @pl.when(col_on)
            def _():
                drain(send_cf.at[g, pl.ds(0, 5)], out_sems.at[11 + g])

            @pl.when(jnp.logical_not(col_on))
            def _():
                drain(send_cf.at[g, pl.ds(0, 6)], out_sems.at[11 + g])

    @pl.when(jnp.logical_not(row_on))
    def _():
        for t in range(5):
            drain(send_rf.at[t, pl.ds(0, ROWS)], out_sems.at[6 + t])


def post_kernel(place, offset, scal, block, velocity, accumulator, new_velocity, new_accumulator):
    step = pl.program_id(0)
    drift = scal[1] * scal[2]
    hats = [(block[g, :N], block[g, N:]) for g in range(4)]
    lane = lax.broadcasted_iota(jnp.int32, (N, 128), 1)
    kx_index = lane // 32 + (place[0] * 8 + step * 4)
    kz_index = lane % 32 + place[1] * 32
    ky_index = lax.broadcasted_iota(jnp.int32, (N, 128), 0)
    kx, k1, kz, square, mask = modes(kx_index, kz_index, ky_index, drift)
    flat = kx * kx + kz * kz
    origin = flat == 0.0
    over_square = 1.0 / jnp.maximum(square, 1.0)
    over_flat = 1.0 / jnp.maximum(flat, 1.0)
    result = [[None, None] for _ in range(3)]
    for p in range(2):
        sign = -1.0 if p == 0 else 1.0
        x, q, r, s = [sign * hats[g][1 - p] for g in range(4)]
        v = ((k1 * k1 - flat) * x + k1 * q) * over_square
        w = 0.0 - (r + k1 * s)
        part = [
            jnp.where(origin, 0.0 - k1 * x, (kz * w - kx * k1 * v) * over_flat),
            jnp.where(origin, 0.0, v),
            jnp.where(origin, 0.0 - k1 * s, (0.0 - kx * w - kz * k1 * v) * over_flat),
        ]
        for c in range(3):
            result[c][p] = jnp.where(mask, part[c], 0.0).T
    for i in range(4):
        shift = (0 - offset[step * 4 + i]) & (N - 1)
        kx_index = jnp.full((32, N), place[0] * 8 + step * 4 + i, jnp.int32)
        kz_index = lax.broadcasted_iota(jnp.int32, (32, N), 0) + place[1] * 32
        ky_index = lax.broadcasted_iota(jnp.int32, (32, N), 1)
        kx, k1, kz, square, _ = modes(kx_index, kz_index, ky_index, drift)
        wave = (kx, k1, kz)
        coupling = 2.0 * scal[1] * kx / jnp.maximum(square, 1.0)
        damp = scal[0] * square
        for p in range(2):
            v = [pltpu.roll(velocity[c, p, i], shift, 1) for c in range(3)]
            for c in range(3):
                rate = result[c][p][32 * i:32 * i + 32] + coupling * wave[c] * v[1] - damp * v[c]
                if c == 0:
                    rate = rate - scal[1] * v[1]
                fresh = (-5.0 / 9.0) * pltpu.roll(accumulator[c, p, i], shift, 1) + scal[3] * rate
                new_accumulator[c, p, i] = fresh
                new_velocity[c, p, i] = v[c] + (15.0 / 16.0) * fresh


def call(kernel, grid, ins, outs, scratch=()):
    return pl.pallas_call(
        kernel,
        grid=grid,
        in_specs=ins,
        out_specs=[spec for spec, _ in outs],
        out_shape=[shape for _, shape in outs],
        scratch_shapes=list(scratch),
        compiler_params=pltpu.CompilerParams(vmem_limit_bytes=VLIM),
    )


def spec(shape, index):
    return pl.BlockSpec(shape, index)


def whole(array):
    rank = array.ndim
    return pl.BlockSpec(array.shape, lambda *_: (0,) * rank)


SMEM = pl.BlockSpec(memory_space=pltpu.SMEM)


def body(velocity, accumulator, remesh_flag, remesh_shift, viscosity, shear, clock, step):
    first, second, back, fore = [jnp.asarray(table) for table in tables()]
    place = jnp.stack([lax.axis_index("row"), lax.axis_index("col")]).astype(jnp.int32)
    offset = remesh_flag * remesh_shift
    scal = jnp.concatenate([viscosity, shear, clock, step])
    shape = jax.ShapeDtypeStruct
    high, low, sums = call(
        pre_kernel, (8,),
        [SMEM, SMEM, SMEM, spec((3, 2, 1, 32, N), lambda i: (0, 0, i, 0, 0))],
        [(spec((3, 32, 2 * N), lambda i: (0, i, 0)), shape((3, N, 2 * N), BF16)),
         (spec((3, 32, 2 * N), lambda i: (0, i, 0)), shape((3, N, 2 * N), BF16)),
         (spec((8, N), lambda i: (0, 0)), shape((8, N), F32))],
    )(place, offset, scal, velocity)
    vmem = pl.BlockSpec(memory_space=pltpu.VMEM)
    hats, total = pl.pallas_call(
        middle_kernel,
        in_specs=[vmem] * 7,
        out_specs=[vmem] * 2,
        out_shape=[shape((4, 2 * N, N), F32), shape((8, N), F32)],
        scratch_shapes=[
            pltpu.VMEM((3, 8, 2, 32, N), F32), pltpu.VMEM((3, 8, 2, 32, N), F32),
            pltpu.VMEM((3, 16, 2, 8, 2 * N), F32), pltpu.VMEM((3, 16, 2, 8, 2 * N), F32),
            pltpu.VMEM((5, 16, 2, 8, 2 * N), F32), pltpu.VMEM((5, 16, 2, 8, 2 * N), F32),
            pltpu.VMEM((4, 8, 2, 32, N), F32), pltpu.VMEM((4, 8, 2, 32, N), F32),
            pltpu.VMEM((8, 8, N), F32),
            pltpu.VMEM((3, N, 2 * N), F32), pltpu.VMEM((5, N, 2 * N), F32), pltpu.VMEM((4, N, 128), F32),
            pltpu.SemaphoreType.DMA((16,)), pltpu.SemaphoreType.DMA((16,)),
        ],
        compiler_params=pltpu.CompilerParams(collective_id=0, has_side_effects=True, vmem_limit_bytes=VLIM),
    )(high, low, sums, first, second, back, fore)
    state = spec((3, 2, 4, 32, N), lambda i: (0, 0, i, 0, 0))
    new_velocity, new_accumulator = call(
        post_kernel, (2,),
        [SMEM, SMEM, SMEM, spec((4, 2 * N, 128), lambda i: (0, 0, i)), state, state],
        [(state, shape(velocity.shape, F32)), (state, shape(velocity.shape, F32))],
    )(place, offset, scal, hats, velocity, accumulator)
    total = jnp.sum(total.reshape(8, 2, 128), axis=2)
    scale = jnp.stack([jnp.ones((), F32), 2.0 * viscosity[0]]) / (N * N)
    return new_velocity, new_accumulator, total.T * scale[:, None]


def solution(mesh):
    state = P(None, None, "row", "col", None)
    return jax.shard_map(
        body,
        mesh=mesh,
        in_specs=(state, state, P("row"), P("row"), P(), P(), P(), P()),
        out_specs=(state, state, P(None, "row")),
        check_vma=False,
    )
```

```python
import numpy as np
import jax
import jax.numpy as jnp
from jax import lax
from jax.experimental import pallas as pl
from jax.experimental.pallas import tpu as pltpu
from jax.sharding import PartitionSpec as P

N = 256
ROWS = 11
COLS = (0, 1, 2, 5, 6, 7)
KX = 8 * ROWS
F32 = jnp.float32
BF16 = jnp.bfloat16
VLIM = 60 * 1024 * 1024


def halves(table):
    table = table.astype(np.float32)
    high = table.astype(jnp.bfloat16)
    low = (table - high.astype(np.float32)).astype(jnp.bfloat16)
    return np.stack([high, low])


def tables():
    index = np.arange(N)
    angle = (index[:, None] * index[None, :] % N) * (2.0 * np.pi / N)
    cos, sin = np.cos(angle) / 16.0, np.sin(angle) / 16.0
    first = np.block([[cos, -sin], [sin, cos]])
    second = np.block([[cos, sin], [-sin, cos]])
    place = np.arange(KX)
    order = 4 * (place % 22) + place // 22
    weights = np.where(order == 0, 1.0, 2.0)
    back_x = np.concatenate([cos[:, order] * weights, -sin[:, order] * weights], axis=1)
    fore_x = np.concatenate([cos[order], -sin[order]], axis=0)
    return halves(first), halves(second), halves(back_x), halves(fore_x)


def split(value):
    high = value.astype(BF16)
    return high, (value - high.astype(F32)).astype(BF16)


def dot3(left, right, dims=((1,), (0,))):
    def one(a, b):
        return lax.dot_general(a, b, (dims, ((), ())), preferred_element_type=F32)

    return one(left[0], right[0]) + one(left[1], right[0]) + one(left[0], right[1])


def swap_chunks(items, width):
    items = list(items)
    count = len(items)
    lane = lax.broadcasted_iota(jnp.int32, items[0].shape, items[0].ndim - 1) // width
    axis = items[0].ndim - 1
    step = count // 2
    while step:
        keep = (lane & step) == 0
        for i in range(count):
            if i & step == 0:
                a, b = items[i], items[i + step]
                items[i] = jnp.where(keep, a, pltpu.roll(b, step * width, axis))
                items[i + step] = jnp.where(keep, pltpu.roll(a, 128 - step * width, axis), b)
        step //= 2
    return items


def signed(index):
    return jnp.where(2 * index < N, index, index - N)


def modes(kx_index, kz_index, ky_index, drift):
    wave_x = kx_index.astype(F32)
    wave_z = signed(kz_index).astype(F32)
    wave_y = signed(ky_index).astype(F32) - drift * wave_x
    square = wave_x * wave_x + wave_y * wave_y + wave_z * wave_z
    mask = (3 * kx_index < N) & (3 * jnp.abs(signed(kz_index)) < N) & (3 * jnp.abs(signed(ky_index)) < N)
    return wave_x, wave_y, wave_z, square, mask


def pre_kernel(flag, amount, shear, clock, velocity, high_out, low_out, sums_out):
    step = pl.program_id(0)
    shift = (0 - flag[step] * amount[step]) & (N - 1)
    kx = jnp.full((32, N), lax.axis_index("row") * 8 + step, jnp.int32)
    kz = lax.broadcasted_iota(jnp.int32, (32, N), 0) + lax.axis_index("col") * 32
    ky = lax.broadcasted_iota(jnp.int32, (32, N), 1)
    wave_x, wave_y, wave_z, square, mask = modes(kx, kz, ky, shear[0] * clock[0])
    inverse = 1.0 / jnp.maximum(square, 1.0)
    wave = (wave_x, wave_y, wave_z)
    energy = jnp.zeros((32, N), F32)
    stress = jnp.zeros((32, N), F32)
    for p in range(2):
        v = [pltpu.roll(velocity[c, p, 0], shift, 1) for c in range(3)]
        energy += v[0] * v[0] + v[1] * v[1] + v[2] * v[2]
        stress += v[0] * v[1]
        along = (wave[0] * v[0] + wave[1] * v[1] + wave[2] * v[2]) * inverse
        for c in range(3):
            high, low = split(jnp.where(mask, v[c] - wave[c] * along, 0.0))
            high_out[c, :, p * N:(p + 1) * N] = high
            low_out[c, :, p * N:(p + 1) * N] = low
    def total(value):
        value = jnp.sum(value, axis=0, keepdims=True)
        return value[:, :128] + value[:, 128:]
    sums_out[pl.ds(step, 1), :] = jnp.concatenate([total(stress), total(square * energy)], axis=1)


MESH = pl.DeviceIdType.MESH


def middle_kernel(high, low, sums, first, second, back, fore, hats_out, total_out,
                  send_b, recv_b, send_f, recv_f, recv_s, u, hats, data, out_sems, in_sems):
    row, col = lax.axis_index("row"), lax.axis_index("col")
    me = row * 8 + col
    on = (row < ROWS) & (col != 3) & (col != 4)
    off = jnp.logical_not(on)

    def push(src, dst, sem, device):
        return pltpu.make_async_remote_copy(
            src_ref=src, dst_ref=dst, send_sem=out_sems.at[sem], recv_sem=in_sems.at[sem],
            device_id=device, device_id_type=MESH)

    def drain(blocks, sem):
        ref = recv_f.at[0, pl.ds(0, 8 * blocks)]
        pltpu.make_async_copy(ref, ref, sem).wait()

    barrier = pltpu.get_barrier_semaphore()

    def greet(i, carry):
        to = lax.rem(me + i, 128)
        pl.semaphore_signal(barrier, inc=1, device_id={"row": to // 8, "col": lax.rem(to, 8)}, device_id_type=MESH)
        return carry

    lax.fori_loop(1, 128, greet, 0)
    pl.semaphore_wait(barrier, 127)
    for i in range(1, 8):
        push(sums, recv_s.at[col], 7, {"col": (col + i) % 8}).start()

    @pl.when(on)
    def _():
        def y_back(f, carry):
            result = dot3((first[0], first[1]), (high[f], low[f]), ((1,), (1,)))
            for h in range(2):
                for plane in range(2):
                    for p in range(2):
                        start = p * N + plane * 128
                        send_b[f, pl.ds((h * 2 + plane) * 2 + p, 128, stride=8), :] = (
                            result[start:start + 128, 128 * h:128 * h + 128])

            def send(i, carry):
                to = lax.rem(me + i, 128)
                push(send_b.at[f, pl.ds(to * 8, 8)], recv_b.at[f, col, pl.ds(row * 8, 8)], f,
                     {"row": to // 8, "col": lax.rem(to, 8)}).start()
                return carry

            lax.fori_loop(1, 128, send, 0)
            recv_b[f, col, pl.ds(row * 8, 8), :] = send_b[f, pl.ds(me * 8, 8), :]
            return carry

        lax.fori_loop(0, 3, y_back, 0)

    def to_grid(f):
        @pl.when(on)
        def _():
            drain(65, in_sems.at[f])

        @pl.when(off)
        def _():
            drain(66, in_sems.at[f])

        for g in range(2):
            blocks = [recv_b[f, c] if c in COLS else jnp.zeros((KX, 128), F32) for c in range(4 * g, 4 * g + 4)]
            moved = swap_chunks(blocks, 32)
            for i in range(4):
                data[g, KX * i:KX * i + KX, :] = moved[i]
        modes_in = jnp.concatenate(
            [jnp.concatenate([data[g, pl.ds(plane * 2 + p, KX, stride=4), :] for p in range(2) for g in range(2)], axis=1)
             for plane in range(2)], axis=0)
        lines = dot3(split(modes_in), (second[0], second[1]))
        for plane in range(2):
            both = jnp.concatenate([lines[KX * plane:KX * plane + KX, p * N:p * N + N] for p in range(2)], axis=0)
            u[f, :, plane * N:plane * N + N] = dot3((back[0], back[1]), split(both))

    def to_modes(t):
        a = jnp.where((t == 0) | (t == 3), 0, jnp.where(t == 4, 2, 1))
        b = jnp.where(t < 2, 1, 2)
        weight = jnp.where((t == 1) | (t == 4), 1.0, 0.0)
        planes = []
        for plane in range(2):
            lanes = slice(plane * N, plane * N + N)
            field = u[a, :, lanes] * u[b, :, lanes] - weight * (u[0, :, lanes] * u[0, :, lanes])
            hat = dot3((fore[0], fore[1]), split(field))
            planes.append(jnp.concatenate([hat[:KX], hat[KX:]], axis=1))
        hats[t] = dot3(split(jnp.concatenate(planes, axis=0)), (first[0], first[1]))

    place = lax.broadcasted_iota(jnp.int32, (KX, N), 0)
    group = (place >= 22).astype(jnp.int32) + (place >= 44).astype(jnp.int32) + (place >= 66).astype(jnp.int32)
    kx_index = 4 * (place - 22 * group) + group
    kz_index = lax.broadcasted_iota(jnp.int32, (KX, N), 1)
    kx = kx_index.astype(F32)
    kz = signed(kz_index).astype(F32)
    origin = (kx_index == 0) & (kz_index == 0)

    def field_out(g, formula):
        for plane in range(2):
            for p in range(2):
                value = formula(lambda t: hats[t, plane * KX:plane * KX + KX, p * N:p * N + N])
                for half in range(2):
                    data[half, pl.ds(plane * 2 + p, KX, stride=4), :] = value[:, 128 * half:128 * half + 128]
        for half in range(2):
            moved = swap_chunks([data[half, KX * i:KX * i + KX, :] for i in range(4)], 32)
            for i in range(4):
                if 4 * half + i in COLS:
                    send_f[g, 4 * half + i] = moved[i]

        def send(i, carry):
            number = lax.rem(me + i, 6 * ROWS)
            to_row, spot = number // 6, lax.rem(number, 6)
            to_col = spot + 2 * (spot // 3)

            @pl.when((to_row != row) | (to_col != col))
            def _():
                push(send_f.at[g, to_col, pl.ds(to_row * 8, 8)], recv_f.at[g, pl.ds(me * 8, 8)], 3 + g,
                     {"row": to_row, "col": to_col}).start()

            return carry

        lax.fori_loop(0, 6 * ROWS, send, 0)

        @pl.when(on)
        def _():
            recv_f[g, pl.ds(me * 8, 8), :] = send_f[g, col, pl.ds(row * 8, 8), :]

    def step_of(step, carry):
        backward = (step == 0) | (step == 1) | (step == 4)

        @pl.when(backward)
        def _():
            to_grid(jnp.where(step == 4, 2, jnp.minimum(step, 2)))

        @pl.when(jnp.logical_not(backward))
        def _():
            to_modes(jnp.where(step < 4, step - 2, step - 3))

        @pl.when(step == 5)
        def _():
            field_out(0, lambda t: jnp.where(origin, t(0), kx * t(0) + kz * t(2)))
            field_out(1, lambda t: jnp.where(origin, t(2), kz * t(0) - kx * t(2)))

        @pl.when(step == 7)
        def _():
            field_out(2, lambda t: (kz * kz - kx * kx) * t(3) - kx * kz * t(4))
            field_out(3, lambda t: 2.0 * kx * kz * t(3) + kz * kz * t(4) - (kx * kx + kz * kz) * t(1))

        return carry

    lax.fori_loop(0, 8, step_of, 0)

    drain_sums = recv_s.at[pl.ds(0, 7)]
    pltpu.make_async_copy(drain_sums, drain_sums, in_sems.at[7]).wait()
    recv_s[col] = sums[...]
    total = recv_s[0]
    for i in range(1, 8):
        total = total + recv_s[i]
    total_out[...] = total

    @pl.when(on)
    def _():
        def y_fore(g, carry):
            drain(127, in_sems.at[3 + g])
            both = jnp.concatenate(
                [jnp.concatenate([recv_f[g, pl.ds((h * 2 + plane) * 2 + p, 128, stride=8), :] for h in range(2)], axis=1)
                 for p in range(2) for plane in range(2)], axis=0)
            hats_out[g] = dot3((second[0], second[1]), split(both))
            return carry

        lax.fori_loop(0, 4, y_fore, 0)

    @pl.when(off)
    def _():
        for g in range(4):
            hats_out[g] = jnp.zeros((2 * N, N), F32)

    pltpu.make_async_copy(drain_sums, drain_sums, out_sems.at[7]).wait()

    @pl.when(on)
    def _():
        for f in range(3):
            drain(127, out_sems.at[f])
        for g in range(4):
            drain(65, out_sems.at[3 + g])

    @pl.when(off)
    def _():
        for g in range(4):
            drain(66, out_sems.at[3 + g])


def post_kernel(flag, amount, viscosity, shear, clock, time_step, total, block, velocity, accumulator,
                new_velocity, new_accumulator, spectra):
    step = pl.program_id(0)
    row, col = lax.axis_index("row"), lax.axis_index("col")
    drift = shear[0] * clock[0]

    @pl.when(step == 0)
    def _():
        diagonal = lax.broadcasted_iota(jnp.int32, (8, 8), 0) == lax.broadcasted_iota(jnp.int32, (8, 8), 1)
        for i, factor in enumerate((1.0, 2.0 * viscosity[0])):
            value = jnp.sum(total[:, 128 * i:128 * i + 128], axis=1, keepdims=True) * (factor / (N * N))
            spectra[i:i + 1, :] = jnp.sum(jnp.where(diagonal, value, 0.0), axis=0, keepdims=True)

    hats = [(block[g, :N], block[g, N:]) for g in (0, 3, 2, 1)]
    lane = lax.broadcasted_iota(jnp.int32, (N, 128), 1)
    kx_index = lane // 32 + (row * 8 + step * 4)
    kz_index = lane % 32 + col * 32
    ky_index = lax.broadcasted_iota(jnp.int32, (N, 128), 0)
    kx, k1, kz, square, mask = modes(kx_index, kz_index, ky_index, drift)
    flat = kx * kx + kz * kz
    origin = flat == 0.0
    over_square = 1.0 / jnp.maximum(square, 1.0)
    over_flat = 1.0 / jnp.maximum(flat, 1.0)
    result = [[None, None] for _ in range(3)]
    for p in range(2):
        sign = -1.0 if p == 0 else 1.0
        x, q, r, s = [sign * hats[g][1 - p] for g in range(4)]
        v = ((k1 * k1 - flat) * x + k1 * q) * over_square
        w = 0.0 - (r + k1 * s)
        part = [
            jnp.where(origin, 0.0 - k1 * x, (kz * w - kx * k1 * v) * over_flat),
            jnp.where(origin, 0.0, v),
            jnp.where(origin, 0.0 - k1 * s, (0.0 - kx * w - kz * k1 * v) * over_flat),
        ]
        for c in range(3):
            result[c][p] = jnp.where(mask, part[c], 0.0).T
    for i in range(4):
        shift = (0 - flag[step * 4 + i] * amount[step * 4 + i]) & (N - 1)
        kx_index = jnp.full((32, N), row * 8 + step * 4 + i, jnp.int32)
        kz_index = lax.broadcasted_iota(jnp.int32, (32, N), 0) + col * 32
        ky_index = lax.broadcasted_iota(jnp.int32, (32, N), 1)
        kx, k1, kz, square, _ = modes(kx_index, kz_index, ky_index, drift)
        wave = (kx, k1, kz)
        coupling = 2.0 * shear[0] * kx / jnp.maximum(square, 1.0)
        damp = viscosity[0] * square
        for p in range(2):
            v = [pltpu.roll(velocity[c, p, i], shift, 1) for c in range(3)]
            for c in range(3):
                rate = result[c][p][32 * i:32 * i + 32] + coupling * wave[c] * v[1] - damp * v[c]
                if c == 0:
                    rate = rate - shear[0] * v[1]
                fresh = (-5.0 / 9.0) * pltpu.roll(accumulator[c, p, i], shift, 1) + time_step[0] * rate
                new_accumulator[c, p, i] = fresh
                new_velocity[c, p, i] = v[c] + (15.0 / 16.0) * fresh


def call(kernel, grid, ins, outs, scratch=()):
    return pl.pallas_call(
        kernel,
        grid=grid,
        in_specs=ins,
        out_specs=[spec for spec, _ in outs],
        out_shape=[shape for _, shape in outs],
        scratch_shapes=list(scratch),
        compiler_params=pltpu.CompilerParams(vmem_limit_bytes=VLIM),
    )


def spec(shape, index):
    return pl.BlockSpec(shape, index)


def whole(array):
    rank = array.ndim
    return pl.BlockSpec(array.shape, lambda *_: (0,) * rank)


SMEM = pl.BlockSpec(memory_space=pltpu.SMEM)


def body(velocity, accumulator, remesh_flag, remesh_shift, viscosity, shear, clock, step):
    first, second, back, fore = [jnp.asarray(table) for table in tables()]
    shape = jax.ShapeDtypeStruct
    high, low, sums = call(
        pre_kernel, (8,),
        [SMEM] * 4 + [spec((3, 2, 1, 32, N), lambda i: (0, 0, i, 0, 0))],
        [(spec((3, 32, 2 * N), lambda i: (0, i, 0)), shape((3, N, 2 * N), BF16)),
         (spec((3, 32, 2 * N), lambda i: (0, i, 0)), shape((3, N, 2 * N), BF16)),
         (spec((8, N), lambda i: (0, 0)), shape((8, N), F32))],
    )(remesh_flag, remesh_shift, shear, clock, velocity)
    vmem = pl.BlockSpec(memory_space=pltpu.VMEM)
    hats, total = pl.pallas_call(
        middle_kernel,
        in_specs=[vmem] * 7,
        out_specs=[vmem] * 2,
        out_shape=[shape((4, 2 * N, N), F32), shape((8, N), F32)],
        scratch_shapes=[
            pltpu.VMEM((3, 1024, 128), F32), pltpu.VMEM((3, 8, KX, 128), F32),
            pltpu.VMEM((4, 8, KX, 128), F32), pltpu.VMEM((4, 1024, 128), F32),
            pltpu.VMEM((8, 8, N), F32),
            pltpu.VMEM((3, N, 2 * N), F32), pltpu.VMEM((5, 2 * KX, 2 * N), F32), pltpu.VMEM((2, 4 * KX, 128), F32),
            pltpu.SemaphoreType.DMA((8,)), pltpu.SemaphoreType.DMA((8,)),
        ],
        compiler_params=pltpu.CompilerParams(collective_id=0, has_side_effects=True, vmem_limit_bytes=VLIM),
    )(high, low, sums, first, second, back, fore)
    state = spec((3, 2, 4, 32, N), lambda i: (0, 0, i, 0, 0))
    return call(
        post_kernel, (2,),
        [SMEM] * 6 + [spec((8, N), lambda i: (0, 0)), spec((4, 2 * N, 128), lambda i: (0, 0, i)), state, state],
        [(state, shape(velocity.shape, F32)), (state, shape(velocity.shape, F32)),
         (spec((2, 8), lambda i: (0, 0)), shape((2, 8), F32))],
    )(remesh_flag, remesh_shift, viscosity, shear, clock, step, total, hats, velocity, accumulator)


def solution(mesh):
    state = P(None, None, "row", "col", None)
    return jax.shard_map(
        body,
        mesh=mesh,
        in_specs=(state, state, P("row"), P("row"), P(), P(), P(), P()),
        out_specs=(state, state, P(None, "row")),
        check_vma=False,
    )
```

```python
import numpy as np
import jax
import jax.numpy as jnp
from jax import lax
from jax.experimental import pallas as pl
from jax.experimental.pallas import tpu as pltpu
from jax.sharding import PartitionSpec as P

N = 256
ROWS = 11
COLS = (0, 1, 2, 5, 6, 7)
KX = 8 * ROWS
F32 = jnp.float32
BF16 = jnp.bfloat16
MIB = 1024 * 1024


def halves(table):
    table = table.astype(np.float32)
    high = table.astype(jnp.bfloat16)
    low = (table - high.astype(np.float32)).astype(jnp.bfloat16)
    return np.stack([high, low])


def tables():
    index = np.arange(N)
    angle = (index[:, None] * index[None, :] % N) * (2.0 * np.pi / N)
    cos, sin = np.cos(angle) / 16.0, np.sin(angle) / 16.0
    first = np.block([[cos, -sin], [sin, cos]])
    second = np.block([[cos, sin], [-sin, cos]])
    place = np.arange(KX)
    order = 4 * (place % 22) + place // 22
    weights = np.where(order == 0, 1.0, 2.0)
    back_x = np.concatenate([cos[:, order] * weights, -sin[:, order] * weights], axis=1)
    fore_x = np.concatenate([cos[order], -sin[order]], axis=0)
    return halves(first), halves(second), halves(back_x), halves(fore_x)


def split(value):
    high = value.astype(BF16)
    return high, (value - high.astype(F32)).astype(BF16)


def dot3(left, right, dims=((1,), (0,))):
    def one(a, b):
        return lax.dot_general(a, b, (dims, ((), ())), preferred_element_type=F32)

    return one(left[0], right[0]) + one(left[1], right[0]) + one(left[0], right[1])


def swap_chunks(items, width):
    items = list(items)
    count = len(items)
    lane = lax.broadcasted_iota(jnp.int32, items[0].shape, items[0].ndim - 1) // width
    axis = items[0].ndim - 1
    step = count // 2
    while step:
        keep = (lane & step) == 0
        for i in range(count):
            if i & step == 0:
                a, b = items[i], items[i + step]
                items[i] = jnp.where(keep, a, pltpu.roll(b, step * width, axis))
                items[i + step] = jnp.where(keep, pltpu.roll(a, 128 - step * width, axis), b)
        step //= 2
    return items


def signed(index):
    return jnp.where(2 * index < N, index, index - N)


def modes(kx_index, kz_index, ky_index, drift):
    wave_x = kx_index.astype(F32)
    wave_z = signed(kz_index).astype(F32)
    wave_y = signed(ky_index).astype(F32) - drift * wave_x
    square = wave_x * wave_x + wave_y * wave_y + wave_z * wave_z
    mask = (3 * kx_index < N) & (3 * jnp.abs(signed(kz_index)) < N) & (3 * jnp.abs(signed(ky_index)) < N)
    return wave_x, wave_y, wave_z, square, mask


def pre_kernel(flag, amount, shear, clock, velocity, high_out, low_out, sums_out):
    step = pl.program_id(0)
    shift = (0 - flag[step] * amount[step]) & (N - 1)
    kx = jnp.full((32, N), lax.axis_index("row") * 8 + step, jnp.int32)
    kz = lax.broadcasted_iota(jnp.int32, (32, N), 0) + lax.axis_index("col") * 32
    ky = lax.broadcasted_iota(jnp.int32, (32, N), 1)
    wave_x, wave_y, wave_z, square, mask = modes(kx, kz, ky, shear[0] * clock[0])
    inverse = 1.0 / jnp.maximum(square, 1.0)
    wave = (wave_x, wave_y, wave_z)
    energy = jnp.zeros((32, N), F32)
    stress = jnp.zeros((32, N), F32)
    for p in range(2):
        v = [pltpu.roll(velocity[c, p, 0], shift, 1) for c in range(3)]
        energy += v[0] * v[0] + v[1] * v[1] + v[2] * v[2]
        stress += v[0] * v[1]
        along = (wave[0] * v[0] + wave[1] * v[1] + wave[2] * v[2]) * inverse
        for c in range(3):
            high, low = split(jnp.where(mask, v[c] - wave[c] * along, 0.0))
            slot = (0, 2, 1)[c]
            high_out[slot, :, p * N:(p + 1) * N] = high
            low_out[slot, :, p * N:(p + 1) * N] = low
    def total(value):
        value = jnp.sum(value, axis=0, keepdims=True)
        return value[:, :128] + value[:, 128:]
    sums_out[pl.ds(step, 1), :] = jnp.concatenate([total(stress), total(square * energy)], axis=1)


MESH = pl.DeviceIdType.MESH


def middle_kernel(high, low, sums, first, second, back, fore, hats_out, total_out,
                  send_b, recv_b, send_f, recv_f, recv_s, u, hats, data, out_sems, in_sems):
    row, col = lax.axis_index("row"), lax.axis_index("col")
    me = row * 8 + col
    on = (row < ROWS) & (col != 3) & (col != 4)
    off = jnp.logical_not(on)

    def push(src, dst, sem, device):
        return pltpu.make_async_remote_copy(
            src_ref=src, dst_ref=dst, send_sem=out_sems.at[sem], recv_sem=in_sems.at[sem],
            device_id=device, device_id_type=MESH)

    def drain(blocks, sem):
        ref = recv_f.at[0, pl.ds(0, 8 * blocks)]
        pltpu.make_async_copy(ref, ref, sem).wait()

    to_cols = [lax.rem(col + j, 8) for j in range(8)]
    spots = [lax.rem(col + j, 6) for j in range(6)]
    on_cols = [spot + 2 * (spot // 3) for spot in spots]
    barrier = pltpu.get_barrier_semaphore()

    def greet(i, carry):
        to_row = lax.rem(row + i, 16)
        for j in range(8):
            @pl.when((i > 0) | (j > 0))
            def _():
                pl.semaphore_signal(barrier, inc=1, device_id={"row": to_row, "col": to_cols[j]}, device_id_type=MESH)
        return carry

    lax.fori_loop(0, 16, greet, 0)
    pl.semaphore_wait(barrier, 127)
    for i in range(1, 8):
        push(sums, recv_s.at[col], 7, {"col": (col + i) % 8}).start()

    @pl.when(on)
    def _():
        def y_back(f, carry):
            result = dot3((first[0], first[1]), (high[f], low[f]), ((1,), (1,)))
            for h in range(2):
                for plane in range(2):
                    for p in range(2):
                        start = p * N + plane * 128
                        send_b[f, pl.ds((h * 2 + plane) * 2 + p, 128, stride=8), :] = (
                            result[start:start + 128, 128 * h:128 * h + 128])

            def send(i, carry):
                to_row = lax.rem(row + i, 16)
                for j in range(8):
                    @pl.when((i > 0) | (j > 0))
                    def _():
                        push(send_b.at[f, pl.ds(to_row * 64 + to_cols[j] * 8, 8)],
                             recv_b.at[f, col, pl.ds(row * 8, 8)], f, {"row": to_row, "col": to_cols[j]}).start()
                return carry

            lax.fori_loop(0, 16, send, 0)
            recv_b[f, col, pl.ds(row * 8, 8), :] = send_b[f, pl.ds(me * 8, 8), :]
            return carry

        lax.fori_loop(0, 3, y_back, 0)

    def to_grid(f):
        @pl.when(on)
        def _():
            drain(65, in_sems.at[f])

        @pl.when(off)
        def _():
            drain(66, in_sems.at[f])

        for g in range(2):
            blocks = [recv_b[f, c] if c in COLS else jnp.zeros((KX, 128), F32) for c in range(4 * g, 4 * g + 4)]
            moved = swap_chunks(blocks, 32)
            for i in range(4):
                data[g, KX * i:KX * i + KX, :] = moved[i]
        modes_in = jnp.concatenate(
            [jnp.concatenate([data[g, pl.ds(plane * 2 + p, KX, stride=4), :] for p in range(2) for g in range(2)], axis=1)
             for plane in range(2)], axis=0)
        lines = dot3(split(modes_in), (second[0], second[1]))
        for plane in range(2):
            both = jnp.concatenate([lines[KX * plane:KX * plane + KX, p * N:p * N + N] for p in range(2)], axis=0)
            u[f, :, plane * N:plane * N + N] = dot3((back[0], back[1]), split(both))

    def to_modes(t):
        a = jnp.where((t == 0) | (t == 2), 0, jnp.where(t == 4, 2, 1))
        b = jnp.where(t < 2, 1, 2)
        weight = jnp.where((t == 1) | (t == 4), 1.0, 0.0)
        planes = []
        for plane in range(2):
            lanes = slice(plane * N, plane * N + N)
            field = u[a, :, lanes] * u[b, :, lanes] - weight * (u[0, :, lanes] * u[0, :, lanes])
            hat = dot3((fore[0], fore[1]), split(field))
            planes.append(jnp.concatenate([hat[:KX], hat[KX:]], axis=1))
        hats[t] = dot3(split(jnp.concatenate(planes, axis=0)), (first[0], first[1]))

    place = lax.broadcasted_iota(jnp.int32, (KX, N), 0)
    group = (place >= 22).astype(jnp.int32) + (place >= 44).astype(jnp.int32) + (place >= 66).astype(jnp.int32)
    kx_index = 4 * (place - 22 * group) + group
    kz_index = lax.broadcasted_iota(jnp.int32, (KX, N), 1)
    kx = kx_index.astype(F32)
    kz = signed(kz_index).astype(F32)
    origin = (kx_index == 0) & (kz_index == 0)

    def field_out(g, formula):
        for plane in range(2):
            for p in range(2):
                value = formula(lambda t: hats[t, plane * KX:plane * KX + KX, p * N:p * N + N])
                for half in range(2):
                    data[half, pl.ds(plane * 2 + p, KX, stride=4), :] = value[:, 128 * half:128 * half + 128]
        for half in range(2):
            moved = swap_chunks([data[half, KX * i:KX * i + KX, :] for i in range(4)], 32)
            for i in range(4):
                if 4 * half + i in COLS:
                    send_f[g, 4 * half + i] = moved[i]

        def send(i, carry):
            to_row = lax.rem(row + i, ROWS)
            for to_col in on_cols:
                @pl.when((to_row != row) | (to_col != col))
                def _():
                    push(send_f.at[g, to_col, pl.ds(to_row * 8, 8)], recv_f.at[g, pl.ds(me * 8, 8)], 3 + g,
                         {"row": to_row, "col": to_col}).start()
            return carry

        lax.fori_loop(0, ROWS, send, 0)

        @pl.when(on)
        def _():
            recv_f[g, pl.ds(me * 8, 8), :] = send_f[g, col, pl.ds(row * 8, 8), :]

    def step_of(step, carry):
        backward = (step == 0) | (step == 1) | (step == 4)

        @pl.when(backward)
        def _():
            to_grid(jnp.where(step == 4, 2, jnp.minimum(step, 2)))

        @pl.when(jnp.logical_not(backward))
        def _():
            to_modes(jnp.where(step < 4, step - 2, step - 3))

        @pl.when(step == 3)
        def _():
            field_out(0, lambda t: (kz * kz - kx * kx) * t(0) - kx * kz * t(1))

        @pl.when(step == 6)
        def _():
            field_out(1, lambda t: jnp.where(origin, t(2), kx * t(2) + kz * t(3)))
            field_out(2, lambda t: jnp.where(origin, t(3), kz * t(2) - kx * t(3)))

        @pl.when(step == 7)
        def _():
            field_out(3, lambda t: 2.0 * kx * kz * t(0) + kz * kz * t(1) - (kx * kx + kz * kz) * t(4))

        return carry

    lax.fori_loop(0, 8, step_of, 0)

    drain_sums = recv_s.at[pl.ds(0, 7)]
    pltpu.make_async_copy(drain_sums, drain_sums, in_sems.at[7]).wait()
    recv_s[col] = sums[...]
    total = recv_s[0]
    for i in range(1, 8):
        total = total + recv_s[i]
    total_out[...] = total

    @pl.when(on)
    def _():
        def y_fore(g, carry):
            drain(127, in_sems.at[3 + g])
            both = jnp.concatenate(
                [jnp.concatenate([recv_f[g, pl.ds((h * 2 + plane) * 2 + p, 128, stride=8), :] for h in range(2)], axis=1)
                 for p in range(2) for plane in range(2)], axis=0)
            hats_out[g] = dot3((second[0], second[1]), split(both))
            return carry

        lax.fori_loop(0, 4, y_fore, 0)

    @pl.when(off)
    def _():
        for g in range(4):
            hats_out[g] = jnp.zeros((2 * N, N), F32)

    pltpu.make_async_copy(drain_sums, drain_sums, out_sems.at[7]).wait()

    @pl.when(on)
    def _():
        for f in range(3):
            drain(127, out_sems.at[f])
        for g in range(4):
            drain(65, out_sems.at[3 + g])

    @pl.when(off)
    def _():
        for g in range(4):
            drain(66, out_sems.at[3 + g])


def post_kernel(flag, amount, viscosity, shear, clock, time_step, total, block, velocity, accumulator,
                new_velocity, new_accumulator, spectra):
    step = pl.program_id(0)
    row, col = lax.axis_index("row"), lax.axis_index("col")
    drift = shear[0] * clock[0]

    @pl.when(step == 0)
    def _():
        diagonal = lax.broadcasted_iota(jnp.int32, (8, 8), 0) == lax.broadcasted_iota(jnp.int32, (8, 8), 1)
        for i, factor in enumerate((1.0, 2.0 * viscosity[0])):
            value = jnp.sum(total[:, 128 * i:128 * i + 128], axis=1, keepdims=True) * (factor / (N * N))
            spectra[i:i + 1, :] = jnp.sum(jnp.where(diagonal, value, 0.0), axis=0, keepdims=True)

    hats = [(block[g, :N], block[g, N:]) for g in (1, 3, 0, 2)]
    lane = lax.broadcasted_iota(jnp.int32, (N, 128), 1)
    kx_index = lane // 32 + (row * 8 + step * 4)
    kz_index = lane % 32 + col * 32
    ky_index = lax.broadcasted_iota(jnp.int32, (N, 128), 0)
    kx, k1, kz, square, mask = modes(kx_index, kz_index, ky_index, drift)
    flat = kx * kx + kz * kz
    origin = flat == 0.0
    over_square = 1.0 / jnp.maximum(square, 1.0)
    over_flat = 1.0 / jnp.maximum(flat, 1.0)
    result = [[None, None] for _ in range(3)]
    for p in range(2):
        sign = -1.0 if p == 0 else 1.0
        x, q, r, s = [sign * hats[g][1 - p] for g in range(4)]
        v = ((k1 * k1 - flat) * x + k1 * q) * over_square
        w = 0.0 - (r + k1 * s)
        part = [
            jnp.where(origin, 0.0 - k1 * x, (kz * w - kx * k1 * v) * over_flat),
            jnp.where(origin, 0.0, v),
            jnp.where(origin, 0.0 - k1 * s, (0.0 - kx * w - kz * k1 * v) * over_flat),
        ]
        for c in range(3):
            result[c][p] = jnp.where(mask, part[c], 0.0).T
    for i in range(4):
        shift = (0 - flag[step * 4 + i] * amount[step * 4 + i]) & (N - 1)
        kx_index = jnp.full((32, N), row * 8 + step * 4 + i, jnp.int32)
        kz_index = lax.broadcasted_iota(jnp.int32, (32, N), 0) + col * 32
        ky_index = lax.broadcasted_iota(jnp.int32, (32, N), 1)
        kx, k1, kz, square, _ = modes(kx_index, kz_index, ky_index, drift)
        wave = (kx, k1, kz)
        coupling = 2.0 * shear[0] * kx / jnp.maximum(square, 1.0)
        damp = viscosity[0] * square
        for p in range(2):
            v = [pltpu.roll(velocity[c, p, i], shift, 1) for c in range(3)]
            for c in range(3):
                rate = result[c][p][32 * i:32 * i + 32] + coupling * wave[c] * v[1] - damp * v[c]
                if c == 0:
                    rate = rate - shear[0] * v[1]
                fresh = (-5.0 / 9.0) * pltpu.roll(accumulator[c, p, i], shift, 1) + time_step[0] * rate
                new_accumulator[c, p, i] = fresh
                new_velocity[c, p, i] = v[c] + (15.0 / 16.0) * fresh


def call(kernel, grid, limit, ins, outs, scratch=()):
    return pl.pallas_call(
        kernel,
        grid=grid,
        in_specs=ins,
        out_specs=[spec for spec, _ in outs],
        out_shape=[shape for _, shape in outs],
        scratch_shapes=list(scratch),
        compiler_params=pltpu.CompilerParams(vmem_limit_bytes=limit * MIB),
    )


def spec(shape, index):
    return pl.BlockSpec(shape, index)


def whole(array):
    rank = array.ndim
    return pl.BlockSpec(array.shape, lambda *_: (0,) * rank)


SMEM = pl.BlockSpec(memory_space=pltpu.SMEM)


def body(velocity, accumulator, remesh_flag, remesh_shift, viscosity, shear, clock, step):
    first, second, back, fore = [jnp.asarray(table) for table in tables()]
    shape = jax.ShapeDtypeStruct
    high, low, sums = call(
        pre_kernel, (8,), 8,
        [SMEM] * 4 + [spec((3, 2, 1, 32, N), lambda i: (0, 0, i, 0, 0))],
        [(spec((3, 32, 2 * N), lambda i: (0, i, 0)), shape((3, N, 2 * N), BF16)),
         (spec((3, 32, 2 * N), lambda i: (0, i, 0)), shape((3, N, 2 * N), BF16)),
         (spec((8, N), lambda i: (0, 0)), shape((8, N), F32))],
    )(remesh_flag, remesh_shift, shear, clock, velocity)
    vmem = pl.BlockSpec(memory_space=pltpu.VMEM)
    hats, total = pl.pallas_call(
        middle_kernel,
        in_specs=[vmem] * 7,
        out_specs=[vmem] * 2,
        out_shape=[shape((4, 2 * N, N), F32), shape((8, N), F32)],
        scratch_shapes=[
            pltpu.VMEM((3, 1024, 128), F32), pltpu.VMEM((3, 8, KX, 128), F32),
            pltpu.VMEM((4, 8, KX, 128), F32), pltpu.VMEM((4, 1024, 128), F32),
            pltpu.VMEM((8, 8, N), F32),
            pltpu.VMEM((3, N, 2 * N), F32), pltpu.VMEM((5, 2 * KX, 2 * N), F32), pltpu.VMEM((2, 4 * KX, 128), F32),
            pltpu.SemaphoreType.DMA((8,)), pltpu.SemaphoreType.DMA((8,)),
        ],
        compiler_params=pltpu.CompilerParams(collective_id=0, has_side_effects=True, vmem_limit_bytes=32 * MIB),
    )(high, low, sums, first, second, back, fore)
    state = spec((3, 2, 4, 32, N), lambda i: (0, 0, i, 0, 0))
    return call(
        post_kernel, (2,), 20,
        [SMEM] * 6 + [spec((8, N), lambda i: (0, 0)), spec((4, 2 * N, 128), lambda i: (0, 0, i)), state, state],
        [(state, shape(velocity.shape, F32)), (state, shape(velocity.shape, F32)),
         (spec((2, 8), lambda i: (0, 0)), shape((2, 8), F32))],
    )(remesh_flag, remesh_shift, viscosity, shear, clock, step, total, hats, velocity, accumulator)


def solution(mesh):
    state = P(None, None, "row", "col", None)
    return jax.shard_map(
        body,
        mesh=mesh,
        in_specs=(state, state, P("row"), P("row"), P(), P(), P(), P()),
        out_specs=(state, state, P(None, "row")),
        check_vma=False,
    )
```

```python
import numpy as np
import jax
import jax.numpy as jnp
from jax import lax
from jax.experimental import pallas as pl
from jax.experimental.pallas import tpu as pltpu
from jax.sharding import PartitionSpec as P

N = 256
ROWS = 11
COLS = (0, 1, 2, 5, 6, 7)
KX = 8 * ROWS
F32 = jnp.float32
BF16 = jnp.bfloat16
MIB = 1024 * 1024


def halves(table):
    table = table.astype(np.float32)
    high = table.astype(jnp.bfloat16)
    low = (table - high.astype(np.float32)).astype(jnp.bfloat16)
    return np.stack([high, low])


def tables():
    index = np.arange(N)
    angle = (index[:, None] * index[None, :] % N) * (2.0 * np.pi / N)
    cos, sin = np.cos(angle) / 16.0, np.sin(angle) / 16.0
    first = np.block([[cos, -sin], [sin, cos]])
    second = np.block([[cos, sin], [-sin, cos]])
    place = np.arange(KX)
    order = 4 * (place % 22) + place // 22
    weights = np.where(order == 0, 1.0, 2.0)
    back_x = np.concatenate([cos[:, order] * weights, -sin[:, order] * weights], axis=1)
    fore_x = np.concatenate([cos[order], -sin[order]], axis=0)
    return halves(first), halves(second), halves(back_x), halves(fore_x)


def split(value):
    high = value.astype(BF16)
    return high, (value - high.astype(F32)).astype(BF16)


def dot3(left, right, dims=((1,), (0,))):
    def one(a, b):
        return lax.dot_general(a, b, (dims, ((), ())), preferred_element_type=F32)

    return one(left[0], right[0]) + one(left[1], right[0]) + one(left[0], right[1])


def swap_chunks(items, width):
    items = list(items)
    count = len(items)
    lane = lax.broadcasted_iota(jnp.int32, items[0].shape, items[0].ndim - 1) // width
    axis = items[0].ndim - 1
    step = count // 2
    while step:
        keep = (lane & step) == 0
        for i in range(count):
            if i & step == 0:
                a, b = items[i], items[i + step]
                items[i] = jnp.where(keep, a, pltpu.roll(b, step * width, axis))
                items[i + step] = jnp.where(keep, pltpu.roll(a, 128 - step * width, axis), b)
        step //= 2
    return items


def signed(index):
    return jnp.where(2 * index < N, index, index - N)


def modes(kx_index, kz_index, ky_index, drift):
    wave_x = kx_index.astype(F32)
    wave_z = signed(kz_index).astype(F32)
    wave_y = signed(ky_index).astype(F32) - drift * wave_x
    square = wave_x * wave_x + wave_y * wave_y + wave_z * wave_z
    mask = (3 * kx_index < N) & (3 * jnp.abs(signed(kz_index)) < N) & (3 * jnp.abs(signed(ky_index)) < N)
    return wave_x, wave_y, wave_z, square, mask


def start_modes(kx_local, row, col, flag, amount, shear, clock, velocity, high, low, sums):
    shift = (0 - flag[kx_local] * amount[kx_local]) & (N - 1)
    kx = jnp.full((32, N), row * 8 + kx_local, jnp.int32)
    kz = lax.broadcasted_iota(jnp.int32, (32, N), 0) + col * 32
    ky = lax.broadcasted_iota(jnp.int32, (32, N), 1)
    wave_x, wave_y, wave_z, square, mask = modes(kx, kz, ky, shear[0] * clock[0])
    inverse = 1.0 / jnp.maximum(square, 1.0)
    wave = (wave_x, wave_y, wave_z)
    energy = jnp.zeros((32, N), F32)
    stress = jnp.zeros((32, N), F32)
    rows = pl.ds(pl.multiple_of(kx_local * 32, 32), 32)
    for p in range(2):
        v = [pltpu.roll(velocity[c, p, kx_local], shift, 1) for c in range(3)]
        energy += v[0] * v[0] + v[1] * v[1] + v[2] * v[2]
        stress += v[0] * v[1]
        along = (wave[0] * v[0] + wave[1] * v[1] + wave[2] * v[2]) * inverse
        for slot, c in enumerate((0, 2, 1)):
            upper, lower = split(jnp.where(mask, v[c] - wave[c] * along, 0.0))
            high[slot, rows, p * N:(p + 1) * N] = upper
            low[slot, rows, p * N:(p + 1) * N] = lower

    def total(value):
        value = jnp.sum(value, axis=0, keepdims=True)
        return value[:, :128] + value[:, 128:]

    sums[pl.ds(kx_local, 1), :] = jnp.concatenate([total(stress), total(square * energy)], axis=1)


MESH = pl.DeviceIdType.MESH


def middle_kernel(flag_in, amount_in, shear, clock, velocity_in, first_in, second_in, back_in, fore_in,
                  hats_out, total_out, flag, amount, velocity, first, second, back, fore, high, low, sums,
                  send_b, recv_b, send_f, recv_f, recv_s, u, hats, data, out_sems, in_sems, load_sems):
    row, col = lax.axis_index("row"), lax.axis_index("col")
    me = row * 8 + col
    on = (row < ROWS) & (col != 3) & (col != 4)
    off = jnp.logical_not(on)

    def push(src, dst, sem, device):
        return pltpu.make_async_remote_copy(
            src_ref=src, dst_ref=dst, send_sem=out_sems.at[sem], recv_sem=in_sems.at[sem],
            device_id=device, device_id_type=MESH)

    def drain(blocks, sem):
        ref = recv_f.at[0, pl.ds(0, 8 * blocks)]
        pltpu.make_async_copy(ref, ref, sem).wait()

    to_cols = [lax.rem(col + j, 8) for j in range(8)]
    spots = [lax.rem(col + j, 6) for j in range(6)]
    on_cols = [spot + 2 * (spot // 3) for spot in spots]
    barrier = pltpu.get_barrier_semaphore()

    def greet(i, carry):
        to_row = lax.rem(row + i, 16)
        for j in range(8):
            @pl.when((i > 0) | (j > 0))
            def _():
                pl.semaphore_signal(barrier, inc=1, device_id={"row": to_row, "col": to_cols[j]}, device_id_type=MESH)
        return carry

    loads = [pltpu.make_async_copy(velocity_in.at[:, :, kx], velocity.at[:, :, kx], load_sems.at[kx]) for kx in range(8)]
    for i, (source, target) in enumerate(((first_in, first), (second_in, second), (back_in, back), (fore_in, fore))):
        loads.append(pltpu.make_async_copy(source, target, load_sems.at[8 + i]))
    for i, (source, target) in enumerate(((flag_in, flag), (amount_in, amount))):
        loads.append(pltpu.make_async_copy(source, target, load_sems.at[12 + i]))
    for load in loads[12:] + loads[:12]:
        load.start()
    lax.fori_loop(0, 16, greet, 0)

    def prepare(kx, carry):
        pltpu.make_async_copy(velocity_in.at[:, :, kx], velocity.at[:, :, kx], load_sems.at[kx]).wait()
        start_modes(kx, row, col, flag, amount, shear, clock, velocity, high, low, sums)
        return carry

    for load in loads[12:]:
        load.wait()
    lax.fori_loop(0, 8, prepare, 0)
    for load in loads[8:12]:
        load.wait()
    pl.semaphore_wait(barrier, 127)
    for i in range(1, 8):
        push(sums, recv_s.at[col], 7, {"col": (col + i) % 8}).start()

    @pl.when(on)
    def _():
        def y_back(f, carry):
            result = dot3((first[0], first[1]), (high[f], low[f]), ((1,), (1,)))
            for h in range(2):
                for plane in range(2):
                    for p in range(2):
                        start = p * N + plane * 128
                        send_b[f, pl.ds((h * 2 + plane) * 2 + p, 128, stride=8), :] = (
                            result[start:start + 128, 128 * h:128 * h + 128])

            def send(i, carry):
                to_row = lax.rem(row + i, 16)
                for j in range(8):
                    @pl.when((i > 0) | (j > 0))
                    def _():
                        push(send_b.at[f, pl.ds(to_row * 64 + to_cols[j] * 8, 8)],
                             recv_b.at[f, col, pl.ds(row * 8, 8)], f, {"row": to_row, "col": to_cols[j]}).start()
                return carry

            lax.fori_loop(0, 16, send, 0)
            recv_b[f, col, pl.ds(row * 8, 8), :] = send_b[f, pl.ds(me * 8, 8), :]
            return carry

        lax.fori_loop(0, 3, y_back, 0)

    def to_grid(f):
        @pl.when(on)
        def _():
            drain(65, in_sems.at[f])

        @pl.when(off)
        def _():
            drain(66, in_sems.at[f])

        for g in range(2):
            blocks = [recv_b[f, c] if c in COLS else jnp.zeros((KX, 128), F32) for c in range(4 * g, 4 * g + 4)]
            moved = swap_chunks(blocks, 32)
            for i in range(4):
                data[g, KX * i:KX * i + KX, :] = moved[i]
        modes_in = jnp.concatenate(
            [jnp.concatenate([data[g, pl.ds(plane * 2 + p, KX, stride=4), :] for p in range(2) for g in range(2)], axis=1)
             for plane in range(2)], axis=0)
        lines = dot3(split(modes_in), (second[0], second[1]))
        for plane in range(2):
            both = jnp.concatenate([lines[KX * plane:KX * plane + KX, p * N:p * N + N] for p in range(2)], axis=0)
            u[f, :, plane * N:plane * N + N] = dot3((back[0], back[1]), split(both))

    def to_modes(t):
        a = jnp.where((t == 0) | (t == 2), 0, jnp.where(t == 4, 2, 1))
        b = jnp.where(t < 2, 1, 2)
        weight = jnp.where((t == 1) | (t == 4), 1.0, 0.0)
        planes = []
        for plane in range(2):
            lanes = slice(plane * N, plane * N + N)
            field = u[a, :, lanes] * u[b, :, lanes] - weight * (u[0, :, lanes] * u[0, :, lanes])
            hat = dot3((fore[0], fore[1]), split(field))
            planes.append(jnp.concatenate([hat[:KX], hat[KX:]], axis=1))
        hats[t] = dot3(split(jnp.concatenate(planes, axis=0)), (first[0], first[1]))

    place = lax.broadcasted_iota(jnp.int32, (KX, N), 0)
    group = (place >= 22).astype(jnp.int32) + (place >= 44).astype(jnp.int32) + (place >= 66).astype(jnp.int32)
    kx_index = 4 * (place - 22 * group) + group
    kz_index = lax.broadcasted_iota(jnp.int32, (KX, N), 1)
    kx = kx_index.astype(F32)
    kz = signed(kz_index).astype(F32)
    origin = (kx_index == 0) & (kz_index == 0)

    def field_out(g, formula):
        for plane in range(2):
            for p in range(2):
                value = formula(lambda t: hats[t, plane * KX:plane * KX + KX, p * N:p * N + N])
                for half in range(2):
                    data[half, pl.ds(plane * 2 + p, KX, stride=4), :] = value[:, 128 * half:128 * half + 128]
        for half in range(2):
            moved = swap_chunks([data[half, KX * i:KX * i + KX, :] for i in range(4)], 32)
            for i in range(4):
                if 4 * half + i in COLS:
                    send_f[g, 4 * half + i] = moved[i]

        def send(i, carry):
            to_row = lax.rem(row + i, ROWS)
            for to_col in on_cols:
                @pl.when((to_row != row) | (to_col != col))
                def _():
                    push(send_f.at[g, to_col, pl.ds(to_row * 8, 8)], recv_f.at[g, pl.ds(me * 8, 8)], 3 + g,
                         {"row": to_row, "col": to_col}).start()
            return carry

        lax.fori_loop(0, ROWS, send, 0)

        @pl.when(on)
        def _():
            recv_f[g, pl.ds(me * 8, 8), :] = send_f[g, col, pl.ds(row * 8, 8), :]

    def step_of(step, carry):
        backward = (step == 0) | (step == 1) | (step == 4)

        @pl.when(backward)
        def _():
            to_grid(jnp.where(step == 4, 2, jnp.minimum(step, 2)))

        @pl.when(jnp.logical_not(backward))
        def _():
            to_modes(jnp.where(step < 4, step - 2, step - 3))

        @pl.when(step == 3)
        def _():
            field_out(0, lambda t: (kz * kz - kx * kx) * t(0) - kx * kz * t(1))

        @pl.when(step == 6)
        def _():
            field_out(1, lambda t: jnp.where(origin, t(2), kx * t(2) + kz * t(3)))
            field_out(2, lambda t: jnp.where(origin, t(3), kz * t(2) - kx * t(3)))

        @pl.when(step == 7)
        def _():
            field_out(3, lambda t: 2.0 * kx * kz * t(0) + kz * kz * t(1) - (kx * kx + kz * kz) * t(4))

        return carry

    lax.fori_loop(0, 8, step_of, 0)

    drain_sums = recv_s.at[pl.ds(0, 7)]
    pltpu.make_async_copy(drain_sums, drain_sums, in_sems.at[7]).wait()
    recv_s[col] = sums[...]
    total = recv_s[0]
    for i in range(1, 8):
        total = total + recv_s[i]
    total_out[...] = total

    @pl.when(on)
    def _():
        def y_fore(g, carry):
            drain(127, in_sems.at[3 + g])
            both = jnp.concatenate(
                [jnp.concatenate([recv_f[g, pl.ds((h * 2 + plane) * 2 + p, 128, stride=8), :] for h in range(2)], axis=1)
                 for p in range(2) for plane in range(2)], axis=0)
            hats_out[g] = dot3((second[0], second[1]), split(both))
            return carry

        lax.fori_loop(0, 4, y_fore, 0)

    @pl.when(off)
    def _():
        for g in range(4):
            hats_out[g] = jnp.zeros((2 * N, N), F32)

    pltpu.make_async_copy(drain_sums, drain_sums, out_sems.at[7]).wait()

    @pl.when(on)
    def _():
        for f in range(3):
            drain(127, out_sems.at[f])
        for g in range(4):
            drain(65, out_sems.at[3 + g])

    @pl.when(off)
    def _():
        for g in range(4):
            drain(66, out_sems.at[3 + g])


def post_kernel(flag, amount, viscosity, shear, clock, time_step, total, block, velocity, accumulator,
                new_velocity, new_accumulator, spectra):
    step = pl.program_id(0)
    row, col = lax.axis_index("row"), lax.axis_index("col")
    drift = shear[0] * clock[0]

    @pl.when(step == 0)
    def _():
        diagonal = lax.broadcasted_iota(jnp.int32, (8, 8), 0) == lax.broadcasted_iota(jnp.int32, (8, 8), 1)
        for i, factor in enumerate((1.0, 2.0 * viscosity[0])):
            value = jnp.sum(total[:, 128 * i:128 * i + 128], axis=1, keepdims=True) * (factor / (N * N))
            spectra[i:i + 1, :] = jnp.sum(jnp.where(diagonal, value, 0.0), axis=0, keepdims=True)

    hats = [(block[g, :N], block[g, N:]) for g in (1, 3, 0, 2)]
    lane = lax.broadcasted_iota(jnp.int32, (N, 128), 1)
    kx_index = lane // 32 + (row * 8 + step * 4)
    kz_index = lane % 32 + col * 32
    ky_index = lax.broadcasted_iota(jnp.int32, (N, 128), 0)
    kx, k1, kz, square, mask = modes(kx_index, kz_index, ky_index, drift)
    flat = kx * kx + kz * kz
    origin = flat == 0.0
    over_square = 1.0 / jnp.maximum(square, 1.0)
    over_flat = 1.0 / jnp.maximum(flat, 1.0)
    result = [[None, None] for _ in range(3)]
    for p in range(2):
        sign = -1.0 if p == 0 else 1.0
        x, q, r, s = [sign * hats[g][1 - p] for g in range(4)]
        v = ((k1 * k1 - flat) * x + k1 * q) * over_square
        w = 0.0 - (r + k1 * s)
        part = [
            jnp.where(origin, 0.0 - k1 * x, (kz * w - kx * k1 * v) * over_flat),
            jnp.where(origin, 0.0, v),
            jnp.where(origin, 0.0 - k1 * s, (0.0 - kx * w - kz * k1 * v) * over_flat),
        ]
        for c in range(3):
            result[c][p] = jnp.where(mask, part[c], 0.0).T
    for i in range(4):
        shift = (0 - flag[step * 4 + i] * amount[step * 4 + i]) & (N - 1)
        kx_index = jnp.full((32, N), row * 8 + step * 4 + i, jnp.int32)
        kz_index = lax.broadcasted_iota(jnp.int32, (32, N), 0) + col * 32
        ky_index = lax.broadcasted_iota(jnp.int32, (32, N), 1)
        kx, k1, kz, square, _ = modes(kx_index, kz_index, ky_index, drift)
        wave = (kx, k1, kz)
        coupling = 2.0 * shear[0] * kx / jnp.maximum(square, 1.0)
        damp = viscosity[0] * square
        for p in range(2):
            v = [pltpu.roll(velocity[c, p, i], shift, 1) for c in range(3)]
            for c in range(3):
                rate = result[c][p][32 * i:32 * i + 32] + coupling * wave[c] * v[1] - damp * v[c]
                if c == 0:
                    rate = rate - shear[0] * v[1]
                fresh = (-5.0 / 9.0) * pltpu.roll(accumulator[c, p, i], shift, 1) + time_step[0] * rate
                new_accumulator[c, p, i] = fresh
                new_velocity[c, p, i] = v[c] + (15.0 / 16.0) * fresh


def call(kernel, grid, limit, ins, outs, scratch=()):
    return pl.pallas_call(
        kernel,
        grid=grid,
        in_specs=ins,
        out_specs=[spec for spec, _ in outs],
        out_shape=[shape for _, shape in outs],
        scratch_shapes=list(scratch),
        compiler_params=pltpu.CompilerParams(vmem_limit_bytes=limit * MIB),
    )


def spec(shape, index):
    return pl.BlockSpec(shape, index)


def whole(array):
    rank = array.ndim
    return pl.BlockSpec(array.shape, lambda *_: (0,) * rank)


SMEM = pl.BlockSpec(memory_space=pltpu.SMEM)


def body(velocity, accumulator, remesh_flag, remesh_shift, viscosity, shear, clock, step):
    first, second, back, fore = [jnp.asarray(table) for table in tables()]
    shape = jax.ShapeDtypeStruct
    vmem = pl.BlockSpec(memory_space=pltpu.VMEM)
    hbm = pl.BlockSpec(memory_space=pltpu.HBM)
    hats, total = pl.pallas_call(
        middle_kernel,
        in_specs=[hbm] * 2 + [SMEM] * 2 + [hbm] * 5,
        out_specs=[vmem] * 2,
        out_shape=[shape((4, 2 * N, N), F32), shape((8, N), F32)],
        scratch_shapes=[
            pltpu.SMEM((8,), jnp.int32), pltpu.SMEM((8,), jnp.int32),
            pltpu.VMEM(velocity.shape, F32), pltpu.VMEM(first.shape, BF16), pltpu.VMEM(second.shape, BF16),
            pltpu.VMEM(back.shape, BF16), pltpu.VMEM(fore.shape, BF16),
            pltpu.VMEM((3, N, 2 * N), BF16), pltpu.VMEM((3, N, 2 * N), BF16), pltpu.VMEM((8, N), F32),
            pltpu.VMEM((3, 1024, 128), F32), pltpu.VMEM((3, 8, KX, 128), F32),
            pltpu.VMEM((4, 8, KX, 128), F32), pltpu.VMEM((4, 1024, 128), F32),
            pltpu.VMEM((8, 8, N), F32),
            pltpu.VMEM((3, N, 2 * N), F32), pltpu.VMEM((5, 2 * KX, 2 * N), F32), pltpu.VMEM((2, 4 * KX, 128), F32),
            pltpu.SemaphoreType.DMA((8,)), pltpu.SemaphoreType.DMA((8,)), pltpu.SemaphoreType.DMA((14,)),
        ],
        compiler_params=pltpu.CompilerParams(collective_id=0, has_side_effects=True, vmem_limit_bytes=60 * MIB),
    )(remesh_flag, remesh_shift, shear, clock, velocity, first, second, back, fore)
    state = spec((3, 2, 4, 32, N), lambda i: (0, 0, i, 0, 0))
    return call(
        post_kernel, (2,), 60,
        [SMEM] * 6 + [spec((8, N), lambda i: (0, 0)), spec((4, 2 * N, 128), lambda i: (0, 0, i)), state, state],
        [(state, shape(velocity.shape, F32)), (state, shape(velocity.shape, F32)),
         (spec((2, 8), lambda i: (0, 0)), shape((2, 8), F32))],
    )(remesh_flag, remesh_shift, viscosity, shear, clock, step, total, hats, velocity, accumulator)


def solution(mesh):
    state = P(None, None, "row", "col", None)
    return jax.shard_map(
        body,
        mesh=mesh,
        in_specs=(state, state, P("row"), P("row"), P(), P(), P(), P()),
        out_specs=(state, state, P(None, "row")),
        check_vma=False,
    )
```

```python
import numpy as np
import jax
import jax.numpy as jnp
from jax import lax
from jax.experimental import pallas as pl
from jax.experimental.pallas import tpu as pltpu
from jax.sharding import PartitionSpec as P

N = 256
ROWS = 11
COLS = (0, 1, 2, 5, 6, 7)
KX = 8 * ROWS
BACK = 2 * 192
F32 = jnp.float32
BF16 = jnp.bfloat16
MIB = 1024 * 1024


def halves(table):
    table = table.astype(np.float32)
    high = table.astype(jnp.bfloat16)
    low = (table - high.astype(np.float32)).astype(jnp.bfloat16)
    return np.stack([high, low])


def tables():
    index = np.arange(N)
    angle = (index[:, None] * index[None, :] % N) * (2.0 * np.pi / N)
    cos, sin = np.cos(angle) / 16.0, np.sin(angle) / 16.0
    first = np.block([[cos, -sin], [sin, cos]])
    second = np.block([[cos, sin], [-sin, cos]])
    place = np.arange(KX)
    order = 4 * (place % 22) + place // 22
    weights = np.where(order == 0, 1.0, 2.0)
    back_x = np.concatenate([cos[:, order] * weights, -sin[:, order] * weights], axis=1)
    fore_x = np.concatenate([cos[order], -sin[order]], axis=0)
    return halves(first), halves(second), halves(back_x), halves(fore_x)


def split(value):
    high = value.astype(BF16)
    return high, (value - high.astype(F32)).astype(BF16)


def dot3(left, right, dims=((1,), (0,))):
    def one(a, b):
        return lax.dot_general(a, b, (dims, ((), ())), preferred_element_type=F32)

    return one(left[0], right[0]) + one(left[1], right[0]) + one(left[0], right[1])


def swap_chunks(items, width):
    items = list(items)
    count = len(items)
    lane = lax.broadcasted_iota(jnp.int32, items[0].shape, items[0].ndim - 1) // width
    axis = items[0].ndim - 1
    step = count // 2
    while step:
        keep = (lane & step) == 0
        for i in range(count):
            if i & step == 0:
                a, b = items[i], items[i + step]
                items[i] = jnp.where(keep, a, pltpu.roll(b, step * width, axis))
                items[i + step] = jnp.where(keep, pltpu.roll(a, 128 - step * width, axis), b)
        step //= 2
    return items


def signed(index):
    return jnp.where(2 * index < N, index, index - N)


def modes(kx_index, kz_index, ky_index, drift):
    wave_x = kx_index.astype(F32)
    wave_z = signed(kz_index).astype(F32)
    wave_y = signed(ky_index).astype(F32) - drift * wave_x
    square = wave_x * wave_x + wave_y * wave_y + wave_z * wave_z
    mask = (3 * kx_index < N) & (3 * jnp.abs(signed(kz_index)) < N) & (3 * jnp.abs(signed(ky_index)) < N)
    return wave_x, wave_y, wave_z, square, mask


def remeshed_modes(kx_local, row, col, flag, amount, shear, clock, velocity):
    shift = (0 - flag[kx_local] * amount[kx_local]) & (N - 1)
    kx = jnp.full((32, N), row * 8 + kx_local, jnp.int32)
    kz = lax.broadcasted_iota(jnp.int32, (32, N), 0) + col * 32
    ky = lax.broadcasted_iota(jnp.int32, (32, N), 1)
    state = [[pltpu.roll(velocity[c, p, kx_local], shift, 1) for c in range(3)] for p in range(2)]
    return state, modes(kx, kz, ky, shear[0] * clock[0])


def project_modes(kx_local, state, waves, high, low):
    wave, square, mask = waves[:3], waves[3], waves[4]
    inverse = 1.0 / jnp.maximum(square, 1.0)
    rows = pl.ds(pl.multiple_of(kx_local * 32, 32), 32)
    for p in range(2):
        v = state[p]
        along = (wave[0] * v[0] + wave[1] * v[1] + wave[2] * v[2]) * inverse
        for slot, c in enumerate((0, 2, 1)):
            upper, lower = split(jnp.where(mask, v[c] - wave[c] * along, 0.0))
            high[slot, rows, p * N:(p + 1) * N] = upper
            low[slot, rows, p * N:(p + 1) * N] = lower


def add_spectra(kx_local, state, waves, sums):
    energy = jnp.zeros((32, N), F32)
    stress = jnp.zeros((32, N), F32)
    for v in state:
        energy += v[0] * v[0] + v[1] * v[1] + v[2] * v[2]
        stress += v[0] * v[1]

    def total(value):
        value = jnp.sum(value, axis=0, keepdims=True)
        return value[:, :128] + value[:, 128:]

    sums[pl.ds(kx_local, 1), :] = jnp.concatenate([total(stress), total(waves[3] * energy)], axis=1)


MESH = pl.DeviceIdType.MESH


def middle_kernel(flag_in, amount_in, shear, clock, velocity_in, first_in, second_in, back_in, fore_in,
                  hats_out, flag, amount, result, velocity, first, second, back, fore, high, low, sums,
                  send_b, recv_b, send_f, recv_f, recv_s, u, hats, data, out_sems, in_sems, load_sems):
    row, col = lax.axis_index("row"), lax.axis_index("col")
    me = row * 8 + col
    on = (row < ROWS) & (col != 3) & (col != 4)
    off = jnp.logical_not(on)

    def push(src, dst, sem, device):
        return pltpu.make_async_remote_copy(
            src_ref=src, dst_ref=dst, send_sem=out_sems.at[sem], recv_sem=in_sems.at[sem],
            device_id=device, device_id_type=MESH)

    def drain(blocks, sem):
        ref = recv_f.at[0, pl.ds(0, 8 * blocks)]
        pltpu.make_async_copy(ref, ref, sem).wait()

    to_cols = [lax.rem(col + j, 8) for j in range(8)]
    spots = [lax.rem(col + j, 6) for j in range(6)]
    on_cols = [spot + 2 * (spot // 3) for spot in spots]
    barrier = pltpu.get_barrier_semaphore()

    def greet(i, carry):
        to_row = lax.rem(row + i, 16)
        for j in range(8):
            @pl.when((i > 0) | (j > 0))
            def _():
                pl.semaphore_signal(barrier, inc=1, device_id={"row": to_row, "col": to_cols[j]}, device_id_type=MESH)
        return carry

    loads = [pltpu.make_async_copy(velocity_in.at[:, :, kx], velocity.at[:, :, kx], load_sems.at[kx]) for kx in range(8)]
    for i, (source, target) in enumerate(((first_in, first), (second_in, second), (back_in, back), (fore_in, fore))):
        loads.append(pltpu.make_async_copy(source, target, load_sems.at[8 + i]))
    for i, (source, target) in enumerate(((flag_in, flag), (amount_in, amount))):
        loads.append(pltpu.make_async_copy(source, target, load_sems.at[12 + i]))
    for load in loads[12:] + loads[:12]:
        load.start()
    lax.fori_loop(0, 16, greet, 0)

    def prepare(kx, carry):
        pltpu.make_async_copy(velocity_in.at[:, :, kx], velocity.at[:, :, kx], load_sems.at[kx]).wait()

        @pl.when(on)
        def _():
            project_modes(kx, *remeshed_modes(kx, row, col, flag, amount, shear, clock, velocity), high, low)

        return carry

    for load in loads[12:]:
        load.wait()
    lax.fori_loop(0, 8, prepare, 0)
    for load in loads[8:12]:
        load.wait()
    pl.semaphore_wait(barrier, 127)
    @pl.when(on)
    def _():
        def y_back(f, carry):
            result = dot3((first[0], first[1]), (high[f], low[f]), ((1,), (1,)))
            for h in range(2):
                for plane in range(2):
                    for p in range(2):
                        start = p * N + plane * 128
                        send_b[f, pl.ds((h * 2 + plane) * 2 + p, 128, stride=8), :] = (
                            result[start:start + 128, 128 * h:128 * h + 128])

            def send(i, carry):
                to_row = lax.rem(row + i, 16)
                for j in range(8):
                    @pl.when((i > 0) | (j > 0))
                    def _():
                        push(send_b.at[f, pl.ds(to_row * 64 + to_cols[j] * 8, 8)],
                             recv_b.at[f, col, pl.ds(row * 8, 8)], f, {"row": to_row, "col": to_cols[j]}).start()
                return carry

            lax.fori_loop(0, 16, send, 0)
            recv_b[f, col, pl.ds(row * 8, 8), :] = send_b[f, pl.ds(me * 8, 8), :]
            return carry

        lax.fori_loop(0, 3, y_back, 0)

    def spectra_of(kx, carry):
        add_spectra(kx, *remeshed_modes(kx, row, col, flag, amount, shear, clock, velocity), sums)
        return carry

    lax.fori_loop(0, 8, spectra_of, 0)
    for i in range(1, 8):
        push(sums, recv_s.at[col], 7, {"col": (col + i) % 8}).start()

    def to_grid(f):
        @pl.when(on)
        def _():
            drain(65, in_sems.at[f])

        @pl.when(off)
        def _():
            drain(66, in_sems.at[f])

        for g in range(2):
            blocks = [recv_b[f, c] if c in COLS else jnp.zeros((KX, 128), F32) for c in range(4 * g, 4 * g + 4)]
            moved = swap_chunks(blocks, 32)
            for i in range(4):
                data[g, KX * i:KX * i + KX, :] = moved[i]
        modes_in = jnp.concatenate(
            [jnp.concatenate([data[g, pl.ds(plane * 2 + p, KX, stride=4), :] for p in range(2) for g in range(2)], axis=1)
             for plane in range(2)], axis=0)
        lines = dot3(split(modes_in), (second[0], second[1]))
        for plane in range(2):
            both = jnp.concatenate([lines[KX * plane:KX * plane + KX, p * N:p * N + N] for p in range(2)], axis=0)
            u[f, :, plane * N:plane * N + N] = dot3((back[0], back[1]), split(both))

    def to_modes(t):
        a = jnp.where((t == 0) | (t == 2), 0, jnp.where(t == 4, 2, 1))
        b = jnp.where(t < 2, 1, 2)
        weight = jnp.where((t == 1) | (t == 4), 1.0, 0.0)
        planes = []
        for plane in range(2):
            lanes = slice(plane * N, plane * N + N)
            field = u[a, :, lanes] * u[b, :, lanes] - weight * (u[0, :, lanes] * u[0, :, lanes])
            hat = dot3((fore[0], fore[1]), split(field))
            planes.append(jnp.concatenate([hat[:KX], hat[KX:]], axis=1))
        hats[t] = dot3(split(jnp.concatenate(planes, axis=0)), (first[0], first[1]))

    place = lax.broadcasted_iota(jnp.int32, (KX, N), 0)
    group = (place >= 22).astype(jnp.int32) + (place >= 44).astype(jnp.int32) + (place >= 66).astype(jnp.int32)
    kx_index = 4 * (place - 22 * group) + group
    kz_index = lax.broadcasted_iota(jnp.int32, (KX, N), 1)
    kx = kx_index.astype(F32)
    kz = signed(kz_index).astype(F32)
    origin = (kx_index == 0) & (kz_index == 0)

    def field_out(g, formula):
        for plane in range(2):
            for p in range(2):
                value = formula(lambda t: hats[t, plane * KX:plane * KX + KX, p * N:p * N + N])
                for half in range(2):
                    data[half, pl.ds(plane * 2 + p, KX, stride=4), :] = value[:, 128 * half:128 * half + 128]
        for half in range(2):
            moved = swap_chunks([data[half, KX * i:KX * i + KX, :] for i in range(4)], 32)
            for i in range(4):
                if 4 * half + i in COLS:
                    send_f[g, 4 * half + i] = moved[i]

        def send(i, carry):
            to_row = lax.rem(row + i, ROWS)
            for to_col in on_cols:
                @pl.when((to_row != row) | (to_col != col))
                def _():
                    push(send_f.at[g, to_col, pl.ds(to_row * 8, 8)], recv_f.at[g, pl.ds(me * 8, 8)], 3 + g,
                         {"row": to_row, "col": to_col}).start()
            return carry

        lax.fori_loop(0, ROWS, send, 0)

        @pl.when(on)
        def _():
            recv_f[g, pl.ds(me * 8, 8), :] = send_f[g, col, pl.ds(row * 8, 8), :]

    def step_of(step, carry):
        backward = (step == 0) | (step == 1) | (step == 4)

        @pl.when(backward)
        def _():
            to_grid(jnp.where(step == 4, 2, jnp.minimum(step, 2)))

        @pl.when(jnp.logical_not(backward))
        def _():
            to_modes(jnp.where(step < 4, step - 2, step - 3))

        @pl.when(step == 3)
        def _():
            field_out(0, lambda t: (kz * kz - kx * kx) * t(0) - kx * kz * t(1))

        @pl.when(step == 6)
        def _():
            field_out(1, lambda t: jnp.where(origin, t(2), kx * t(2) + kz * t(3)))
            field_out(2, lambda t: jnp.where(origin, t(3), kz * t(2) - kx * t(3)))

        @pl.when(step == 7)
        def _():
            field_out(3, lambda t: 2.0 * kx * kz * t(0) + kz * kz * t(1) - (kx * kx + kz * kz) * t(4))

        return carry

    lax.fori_loop(0, 8, step_of, 0)

    drain_sums = recv_s.at[pl.ds(0, 7)]
    pltpu.make_async_copy(drain_sums, drain_sums, in_sems.at[7]).wait()
    recv_s[col] = sums[...]
    total = recv_s[0]
    for i in range(1, 8):
        total = total + recv_s[i]
    for g in range(4):
        result[g, BACK:BACK + 8, :] = total

    @pl.when(on)
    def _():
        def y_fore(g, carry):
            drain(127, in_sems.at[3 + g])
            both = jnp.concatenate(
                [jnp.concatenate([recv_f[g, pl.ds((h * 2 + plane) * 2 + p, 128, stride=8), :] for h in range(2)], axis=1)
                 for p in range(2) for plane in range(2)], axis=0)
            table = [jnp.concatenate([second[i, start:start + 96] for start in (0, 160, 256, 416)], axis=0) for i in range(2)]
            result[g, :BACK, :] = dot3(table, split(both))
            pltpu.make_async_copy(result.at[g], hats_out.at[g], load_sems.at[g]).start()
            return carry

        lax.fori_loop(0, 4, y_fore, 0)

    @pl.when(off)
    def _():
        for g in range(4):
            result[g, :BACK, :] = jnp.zeros((BACK, N), F32)
            pltpu.make_async_copy(result.at[g], hats_out.at[g], load_sems.at[g]).start()

    for g in range(4):
        pltpu.make_async_copy(result.at[g], hats_out.at[g], load_sems.at[g]).wait()

    pltpu.make_async_copy(drain_sums, drain_sums, out_sems.at[7]).wait()

    @pl.when(on)
    def _():
        for f in range(3):
            drain(127, out_sems.at[f])
        for g in range(4):
            drain(65, out_sems.at[3 + g])

    @pl.when(off)
    def _():
        for g in range(4):
            drain(66, out_sems.at[3 + g])


def post_kernel(flag, amount, viscosity, shear, clock, time_step, block, velocity, accumulator,
                new_velocity, new_accumulator, spectra):
    step = pl.program_id(0)
    row, col = lax.axis_index("row"), lax.axis_index("col")
    drift = shear[0] * clock[0]

    diagonal = lax.broadcasted_iota(jnp.int32, (8, 8), 0) == lax.broadcasted_iota(jnp.int32, (8, 8), 1)
    factor = jnp.where(step == 0, 1.0, 2.0 * viscosity[0]) / (N * N)
    value = jnp.sum(block[0, BACK:BACK + 8, :], axis=1, keepdims=True) * factor
    spectra[pl.ds(step, 1), :] = jnp.sum(jnp.where(diagonal, value, 0.0), axis=0, keepdims=True)

    hats = [(block[g, :192], block[g, 192:384]) for g in (1, 3, 0, 2)]
    lane = lax.broadcasted_iota(jnp.int32, (192, 128), 1)
    kx_index = lane // 32 + (row * 8 + step * 4)
    kz_index = lane % 32 + col * 32
    place = lax.broadcasted_iota(jnp.int32, (192, 128), 0)
    ky_index = jnp.where(place < 96, place, place + 64)
    kx, k1, kz, square, mask = modes(kx_index, kz_index, ky_index, drift)
    flat = kx * kx + kz * kz
    origin = flat == 0.0
    over_square = 1.0 / jnp.maximum(square, 1.0)
    over_flat = 1.0 / jnp.maximum(flat, 1.0)
    result = [[None, None] for _ in range(3)]
    for p in range(2):
        sign = -1.0 if p == 0 else 1.0
        x, q, r, s = [sign * hats[g][1 - p] for g in range(4)]
        v = ((k1 * k1 - flat) * x + k1 * q) * over_square
        w = 0.0 - (r + k1 * s)
        part = [
            jnp.where(origin, 0.0 - k1 * x, (kz * w - kx * k1 * v) * over_flat),
            jnp.where(origin, 0.0, v),
            jnp.where(origin, 0.0 - k1 * s, (0.0 - kx * w - kz * k1 * v) * over_flat),
        ]
        for c in range(3):
            kept = jnp.where(mask, part[c], 0.0)
            result[c][p] = jnp.concatenate([kept[:96], jnp.zeros((64, 128), F32), kept[96:]], axis=0).T
    for i in range(4):
        shift = (0 - flag[step * 4 + i] * amount[step * 4 + i]) & (N - 1)
        kx_index = jnp.full((32, N), row * 8 + step * 4 + i, jnp.int32)
        kz_index = lax.broadcasted_iota(jnp.int32, (32, N), 0) + col * 32
        ky_index = lax.broadcasted_iota(jnp.int32, (32, N), 1)
        kx, k1, kz, square, _ = modes(kx_index, kz_index, ky_index, drift)
        wave = (kx, k1, kz)
        coupling = 2.0 * shear[0] * kx / jnp.maximum(square, 1.0)
        damp = viscosity[0] * square
        for p in range(2):
            v = [pltpu.roll(velocity[c, p, i], shift, 1) for c in range(3)]
            for c in range(3):
                rate = result[c][p][32 * i:32 * i + 32] + coupling * wave[c] * v[1] - damp * v[c]
                if c == 0:
                    rate = rate - shear[0] * v[1]
                fresh = (-5.0 / 9.0) * pltpu.roll(accumulator[c, p, i], shift, 1) + time_step[0] * rate
                new_accumulator[c, p, i] = fresh
                new_velocity[c, p, i] = v[c] + (15.0 / 16.0) * fresh


def call(kernel, grid, limit, ins, outs, scratch=()):
    return pl.pallas_call(
        kernel,
        grid=grid,
        in_specs=ins,
        out_specs=[spec for spec, _ in outs],
        out_shape=[shape for _, shape in outs],
        scratch_shapes=list(scratch),
        compiler_params=pltpu.CompilerParams(vmem_limit_bytes=limit * MIB),
    )


def spec(shape, index):
    return pl.BlockSpec(shape, index)


def whole(array):
    rank = array.ndim
    return pl.BlockSpec(array.shape, lambda *_: (0,) * rank)


SMEM = pl.BlockSpec(memory_space=pltpu.SMEM)


def body(velocity, accumulator, remesh_flag, remesh_shift, viscosity, shear, clock, step):
    first, second, back, fore = [jnp.asarray(table) for table in tables()]
    shape = jax.ShapeDtypeStruct
    hbm = pl.BlockSpec(memory_space=pltpu.HBM)
    [hats] = pl.pallas_call(
        middle_kernel,
        in_specs=[hbm] * 2 + [SMEM] * 2 + [hbm] * 5,
        out_specs=[hbm],
        out_shape=[shape((4, BACK + 8, N), F32)],
        scratch_shapes=[
            pltpu.SMEM((8,), jnp.int32), pltpu.SMEM((8,), jnp.int32), pltpu.VMEM((4, BACK + 8, N), F32),
            pltpu.VMEM(velocity.shape, F32), pltpu.VMEM(first.shape, BF16), pltpu.VMEM(second.shape, BF16),
            pltpu.VMEM(back.shape, BF16), pltpu.VMEM(fore.shape, BF16),
            pltpu.VMEM((3, N, 2 * N), BF16), pltpu.VMEM((3, N, 2 * N), BF16), pltpu.VMEM((8, N), F32),
            pltpu.VMEM((3, 1024, 128), F32), pltpu.VMEM((3, 8, KX, 128), F32),
            pltpu.VMEM((4, 8, KX, 128), F32), pltpu.VMEM((4, 1024, 128), F32),
            pltpu.VMEM((8, 8, N), F32),
            pltpu.VMEM((3, N, 2 * N), F32), pltpu.VMEM((5, 2 * KX, 2 * N), F32), pltpu.VMEM((2, 4 * KX, 128), F32),
            pltpu.SemaphoreType.DMA((8,)), pltpu.SemaphoreType.DMA((8,)), pltpu.SemaphoreType.DMA((14,)),
        ],
        compiler_params=pltpu.CompilerParams(collective_id=0, has_side_effects=True, vmem_limit_bytes=60 * MIB),
    )(remesh_flag, remesh_shift, shear, clock, velocity, first, second, back, fore)
    state = spec((3, 2, 4, 32, N), lambda i: (0, 0, i, 0, 0))
    return call(
        post_kernel, (2,), 50,
        [SMEM] * 6 + [spec((4, BACK + 8, 128), lambda i: (0, 0, i)), state, state],
        [(state, shape(velocity.shape, F32)), (state, shape(velocity.shape, F32)),
         (spec((2, 8), lambda i: (0, 0)), shape((2, 8), F32))],
    )(remesh_flag, remesh_shift, viscosity, shear, clock, step, hats, velocity, accumulator)


def solution(mesh):
    state = P(None, None, "row", "col", None)
    return jax.shard_map(
        body,
        mesh=mesh,
        in_specs=(state, state, P("row"), P("row"), P(), P(), P(), P()),
        out_specs=(state, state, P(None, "row")),
        check_vma=False,
    )
```

```python
import numpy as np
import jax
import jax.numpy as jnp
from jax import lax
from jax.experimental import pallas as pl
from jax.experimental.pallas import tpu as pltpu
from jax.sharding import PartitionSpec as P

N = 256
ROWS = 11
COLS = (0, 1, 2, 5, 6, 7)
KX = 8 * ROWS
BACK = 2 * 192
F32 = jnp.float32
BF16 = jnp.bfloat16
MIB = 1024 * 1024


def halves(table):
    table = table.astype(np.float32)
    high = table.astype(jnp.bfloat16)
    low = (table - high.astype(np.float32)).astype(jnp.bfloat16)
    return np.stack([high, low])


def tables():
    index = np.arange(N)
    angle = (index[:, None] * index[None, :] % N) * (2.0 * np.pi / N)
    cos, sin = np.cos(angle) / 16.0, np.sin(angle) / 16.0
    first = np.block([[cos, -sin], [sin, cos]])
    second = np.block([[cos, sin], [-sin, cos]])
    place = np.arange(KX)
    order = 4 * (place % 22) + place // 22
    weights = np.where(order == 0, 1.0, 2.0)
    back_x = np.concatenate([cos[:, order] * weights, -sin[:, order] * weights], axis=1)
    fore_x = np.concatenate([cos[order], -sin[order]], axis=0)
    return halves(first), halves(second), halves(back_x), halves(fore_x)


def split(value):
    high = value.astype(BF16)
    return high, (value - high.astype(F32)).astype(BF16)


def dot3(left, right, dims=((1,), (0,))):
    def one(a, b):
        return lax.dot_general(a, b, (dims, ((), ())), preferred_element_type=F32)

    return one(left[0], right[0]) + one(left[1], right[0]) + one(left[0], right[1])


def swap_chunks(items, width):
    items = list(items)
    count = len(items)
    lane = lax.broadcasted_iota(jnp.int32, items[0].shape, items[0].ndim - 1) // width
    axis = items[0].ndim - 1
    step = count // 2
    while step:
        keep = (lane & step) == 0
        for i in range(count):
            if i & step == 0:
                a, b = items[i], items[i + step]
                items[i] = jnp.where(keep, a, pltpu.roll(b, step * width, axis))
                items[i + step] = jnp.where(keep, pltpu.roll(a, 128 - step * width, axis), b)
        step //= 2
    return items


def signed(index):
    return jnp.where(2 * index < N, index, index - N)


def modes(kx_index, kz_index, ky_index, drift):
    wave_x = kx_index.astype(F32)
    wave_z = signed(kz_index).astype(F32)
    wave_y = signed(ky_index).astype(F32) - drift * wave_x
    square = wave_x * wave_x + wave_y * wave_y + wave_z * wave_z
    mask = (3 * kx_index < N) & (3 * jnp.abs(signed(kz_index)) < N) & (3 * jnp.abs(signed(ky_index)) < N)
    return wave_x, wave_y, wave_z, square, mask


def remeshed_modes(kx_local, row, col, flag, amount, shear, clock, velocity):
    shift = (0 - flag[kx_local] * amount[kx_local]) & (N - 1)
    kx = jnp.full((32, N), row * 8 + kx_local, jnp.int32)
    kz = lax.broadcasted_iota(jnp.int32, (32, N), 0) + col * 32
    ky = lax.broadcasted_iota(jnp.int32, (32, N), 1)
    state = [[pltpu.roll(velocity[c, p, kx_local], shift, 1) for c in range(3)] for p in range(2)]
    return state, modes(kx, kz, ky, shear[0] * clock[0])


def project_modes(kx_local, state, waves, high, low):
    wave, square, mask = waves[:3], waves[3], waves[4]
    inverse = 1.0 / jnp.maximum(square, 1.0)
    rows = pl.ds(pl.multiple_of(kx_local * 32, 32), 32)
    for p in range(2):
        v = state[p]
        along = (wave[0] * v[0] + wave[1] * v[1] + wave[2] * v[2]) * inverse
        for slot, c in enumerate((0, 2, 1)):
            upper, lower = split(jnp.where(mask, v[c] - wave[c] * along, 0.0))
            high[slot, rows, p * N:(p + 1) * N] = upper
            low[slot, rows, p * N:(p + 1) * N] = lower


def add_spectra(kx_local, state, waves, sums):
    energy = jnp.zeros((32, N), F32)
    stress = jnp.zeros((32, N), F32)
    for v in state:
        energy += v[0] * v[0] + v[1] * v[1] + v[2] * v[2]
        stress += v[0] * v[1]

    def total(value):
        value = jnp.sum(value, axis=0, keepdims=True)
        return value[:, :128] + value[:, 128:]

    sums[pl.ds(kx_local, 1), :] = jnp.concatenate([total(stress), total(waves[3] * energy)], axis=1)


MESH = pl.DeviceIdType.MESH


def middle_kernel(flag_in, amount_in, shear, clock, velocity_in, first_in, second_in, back_in, fore_in,
                  hats_out, flag, amount, result, kept, velocity, first, second, back, fore, high, low, sums,
                  send_b, recv_b, send_f, recv_f, recv_s, u, hats, data, out_sems, in_sems, load_sems):
    row, col = lax.axis_index("row"), lax.axis_index("col")
    me = row * 8 + col
    on = (row < ROWS) & (col != 3) & (col != 4)
    off = jnp.logical_not(on)

    def push(src, dst, sem, device):
        return pltpu.make_async_remote_copy(
            src_ref=src, dst_ref=dst, send_sem=out_sems.at[sem], recv_sem=in_sems.at[sem],
            device_id=device, device_id_type=MESH)

    def drain(blocks, sem):
        ref = recv_f.at[0, pl.ds(0, 8 * blocks)]
        pltpu.make_async_copy(ref, ref, sem).wait()

    to_cols = [lax.rem(col + j, 8) for j in range(8)]
    spots = [lax.rem(col + j, 6) for j in range(6)]
    on_cols = [spot + 2 * (spot // 3) for spot in spots]
    barrier = pltpu.get_barrier_semaphore()

    def greet(i, carry):
        to_row = lax.rem(row + i, 16)
        for j in range(8):
            @pl.when((i > 0) | (j > 0))
            def _():
                pl.semaphore_signal(barrier, inc=1, device_id={"row": to_row, "col": to_cols[j]}, device_id_type=MESH)
        return carry

    loads = [pltpu.make_async_copy(velocity_in.at[:, :, kx], velocity.at[:, :, kx], load_sems.at[kx]) for kx in range(8)]
    for i, (source, target) in enumerate(((first_in, first), (second_in, second), (back_in, back), (fore_in, fore))):
        loads.append(pltpu.make_async_copy(source, target, load_sems.at[8 + i]))
    for i, (source, target) in enumerate(((flag_in, flag), (amount_in, amount))):
        loads.append(pltpu.make_async_copy(source, target, load_sems.at[12 + i]))
    for load in loads[12:] + loads[:12]:
        load.start()
    lax.fori_loop(0, 16, greet, 0)

    def prepare(kx, carry):
        pltpu.make_async_copy(velocity_in.at[:, :, kx], velocity.at[:, :, kx], load_sems.at[kx]).wait()

        @pl.when(on)
        def _():
            project_modes(kx, *remeshed_modes(kx, row, col, flag, amount, shear, clock, velocity), high, low)

        return carry

    for load in loads[12:]:
        load.wait()
    lax.fori_loop(0, 8, prepare, 0)
    for load in loads[8:12]:
        load.wait()
    pl.semaphore_wait(barrier, 127)
    @pl.when(on)
    def _():
        def y_back(f, carry):
            result = dot3((first[0], first[1]), (high[f], low[f]), ((1,), (1,)))
            for h in range(2):
                for plane in range(2):
                    for p in range(2):
                        start = p * N + plane * 128
                        send_b[f, pl.ds((h * 2 + plane) * 2 + p, 128, stride=8), :] = (
                            result[start:start + 128, 128 * h:128 * h + 128])

            def send(i, carry):
                to_row = lax.rem(row + i, 16)
                for j in range(8):
                    @pl.when((i > 0) | (j > 0))
                    def _():
                        push(send_b.at[f, pl.ds(to_row * 64 + to_cols[j] * 8, 8)],
                             recv_b.at[f, col, pl.ds(row * 8, 8)], f, {"row": to_row, "col": to_cols[j]}).start()
                return carry

            lax.fori_loop(0, 16, send, 0)
            recv_b[f, col, pl.ds(row * 8, 8), :] = send_b[f, pl.ds(me * 8, 8), :]
            return carry

        lax.fori_loop(0, 3, y_back, 0)

    def spectra_of(kx, carry):
        add_spectra(kx, *remeshed_modes(kx, row, col, flag, amount, shear, clock, velocity), sums)
        return carry

    lax.fori_loop(0, 8, spectra_of, 0)
    for i in range(2):
        for place, start in enumerate((0, 160, 256, 416)):
            kept[i, 96 * place:96 * place + 96, :] = second[i, start:start + 96, :]
    for i in range(1, 8):
        push(sums, recv_s.at[col], 7, {"col": (col + i) % 8}).start()

    def to_grid(f):
        @pl.when(on)
        def _():
            drain(65, in_sems.at[f])

        @pl.when(off)
        def _():
            drain(66, in_sems.at[f])

        for g in range(2):
            blocks = [recv_b[f, c] if c in COLS else jnp.zeros((KX, 128), F32) for c in range(4 * g, 4 * g + 4)]
            moved = swap_chunks(blocks, 32)
            for i in range(4):
                data[g, KX * i:KX * i + KX, :] = moved[i]
        modes_in = jnp.concatenate(
            [jnp.concatenate([data[g, pl.ds(plane * 2 + p, KX, stride=4), :] for p in range(2) for g in range(2)], axis=1)
             for plane in range(2)], axis=0)
        lines = dot3(split(modes_in), (second[0], second[1]))
        for plane in range(2):
            both = jnp.concatenate([lines[KX * plane:KX * plane + KX, p * N:p * N + N] for p in range(2)], axis=0)
            u[f, :, plane * N:plane * N + N] = dot3((back[0], back[1]), split(both))

    def to_modes(t):
        a = jnp.where((t == 0) | (t == 2), 0, jnp.where(t == 4, 2, 1))
        b = jnp.where(t < 2, 1, 2)
        weight = jnp.where((t == 1) | (t == 4), 1.0, 0.0)
        planes = []
        for plane in range(2):
            lanes = slice(plane * N, plane * N + N)
            field = u[a, :, lanes] * u[b, :, lanes] - weight * (u[0, :, lanes] * u[0, :, lanes])
            hat = dot3((fore[0], fore[1]), split(field))
            planes.append(jnp.concatenate([hat[:KX], hat[KX:]], axis=1))
        hats[t] = dot3(split(jnp.concatenate(planes, axis=0)), (first[0], first[1]))

    place = lax.broadcasted_iota(jnp.int32, (KX, N), 0)
    group = (place >= 22).astype(jnp.int32) + (place >= 44).astype(jnp.int32) + (place >= 66).astype(jnp.int32)
    kx_index = 4 * (place - 22 * group) + group
    kz_index = lax.broadcasted_iota(jnp.int32, (KX, N), 1)
    kx = kx_index.astype(F32)
    kz = signed(kz_index).astype(F32)
    origin = (kx_index == 0) & (kz_index == 0)

    def field_out(g, formula):
        for plane in range(2):
            for p in range(2):
                value = formula(lambda t: hats[t, plane * KX:plane * KX + KX, p * N:p * N + N])
                for half in range(2):
                    data[half, pl.ds(plane * 2 + p, KX, stride=4), :] = value[:, 128 * half:128 * half + 128]
        for half in range(2):
            moved = swap_chunks([data[half, KX * i:KX * i + KX, :] for i in range(4)], 32)
            for i in range(4):
                if 4 * half + i in COLS:
                    send_f[g, 4 * half + i] = moved[i]

        def send(i, carry):
            to_row = lax.rem(row + i, ROWS)
            for to_col in on_cols:
                @pl.when((to_row != row) | (to_col != col))
                def _():
                    push(send_f.at[g, to_col, pl.ds(to_row * 8, 8)], recv_f.at[g, pl.ds(me * 8, 8)], 3 + g,
                         {"row": to_row, "col": to_col}).start()
            return carry

        lax.fori_loop(0, ROWS, send, 0)

        @pl.when(on)
        def _():
            recv_f[g, pl.ds(me * 8, 8), :] = send_f[g, col, pl.ds(row * 8, 8), :]

    def step_of(step, carry):
        backward = (step == 0) | (step == 1) | (step == 4)

        @pl.when(backward)
        def _():
            to_grid(jnp.where(step == 4, 2, jnp.minimum(step, 2)))

        @pl.when(jnp.logical_not(backward))
        def _():
            to_modes(jnp.where(step < 4, step - 2, step - 3))

        @pl.when(step == 3)
        def _():
            field_out(0, lambda t: (kz * kz - kx * kx) * t(0) - kx * kz * t(1))

        @pl.when(step == 6)
        def _():
            field_out(1, lambda t: jnp.where(origin, t(2), kx * t(2) + kz * t(3)))
            field_out(2, lambda t: jnp.where(origin, t(3), kz * t(2) - kx * t(3)))

        @pl.when(step == 7)
        def _():
            field_out(3, lambda t: 2.0 * kx * kz * t(0) + kz * kz * t(1) - (kx * kx + kz * kz) * t(4))

        return carry

    lax.fori_loop(0, 8, step_of, 0)

    drain_sums = recv_s.at[pl.ds(0, 7)]
    pltpu.make_async_copy(drain_sums, drain_sums, in_sems.at[7]).wait()
    recv_s[col] = sums[...]
    total = recv_s[0]
    for i in range(1, 8):
        total = total + recv_s[i]
    for g in range(4):
        result[g, BACK:BACK + 8, :] = total

    @pl.when(on)
    def _():
        def y_fore(g, carry):
            drain(127, in_sems.at[3 + g])
            both = jnp.concatenate(
                [jnp.concatenate([recv_f[g, pl.ds((h * 2 + plane) * 2 + p, 128, stride=8), :] for h in range(2)], axis=1)
                 for p in range(2) for plane in range(2)], axis=0)
            result[g, :BACK, :] = dot3((kept[0], kept[1]), split(both))
            pltpu.make_async_copy(result.at[g], hats_out.at[g], load_sems.at[g]).start()
            return carry

        lax.fori_loop(0, 4, y_fore, 0)

    @pl.when(off)
    def _():
        for g in range(4):
            result[g, :BACK, :] = jnp.zeros((BACK, N), F32)
            pltpu.make_async_copy(result.at[g], hats_out.at[g], load_sems.at[g]).start()

    for g in range(4):
        pltpu.make_async_copy(result.at[g], hats_out.at[g], load_sems.at[g]).wait()

    pltpu.make_async_copy(drain_sums, drain_sums, out_sems.at[7]).wait()

    @pl.when(on)
    def _():
        for f in range(3):
            drain(127, out_sems.at[f])
        for g in range(4):
            drain(65, out_sems.at[3 + g])

    @pl.when(off)
    def _():
        for g in range(4):
            drain(66, out_sems.at[3 + g])


def post_kernel(flag, amount, viscosity, shear, clock, time_step, block, velocity, accumulator,
                new_velocity, new_accumulator, spectra):
    step = pl.program_id(0)
    row, col = lax.axis_index("row"), lax.axis_index("col")
    drift = shear[0] * clock[0]

    diagonal = lax.broadcasted_iota(jnp.int32, (8, 8), 0) == lax.broadcasted_iota(jnp.int32, (8, 8), 1)
    factor = jnp.where(step == 0, 1.0, 2.0 * viscosity[0]) / (N * N)
    value = jnp.sum(block[0, BACK:BACK + 8, :], axis=1, keepdims=True) * factor
    spectra[pl.ds(step, 1), :] = jnp.sum(jnp.where(diagonal, value, 0.0), axis=0, keepdims=True)

    hats = [(block[g, :192], block[g, 192:384]) for g in (1, 3, 0, 2)]
    lane = lax.broadcasted_iota(jnp.int32, (192, 128), 1)
    kx_index = lane // 32 + (row * 8 + step * 4)
    kz_index = lane % 32 + col * 32
    place = lax.broadcasted_iota(jnp.int32, (192, 128), 0)
    ky_index = jnp.where(place < 96, place, place + 64)
    kx, k1, kz, square, mask = modes(kx_index, kz_index, ky_index, drift)
    flat = kx * kx + kz * kz
    origin = flat == 0.0
    over_square = 1.0 / jnp.maximum(square, 1.0)
    over_flat = 1.0 / jnp.maximum(flat, 1.0)
    result = [[None, None] for _ in range(3)]
    for p in range(2):
        sign = -1.0 if p == 0 else 1.0
        x, q, r, s = [sign * hats[g][1 - p] for g in range(4)]
        v = ((k1 * k1 - flat) * x + k1 * q) * over_square
        w = 0.0 - (r + k1 * s)
        part = [
            jnp.where(origin, 0.0 - k1 * x, (kz * w - kx * k1 * v) * over_flat),
            jnp.where(origin, 0.0, v),
            jnp.where(origin, 0.0 - k1 * s, (0.0 - kx * w - kz * k1 * v) * over_flat),
        ]
        for c in range(3):
            kept = jnp.where(mask, part[c], 0.0)
            result[c][p] = jnp.concatenate([kept[:96], jnp.zeros((64, 128), F32), kept[96:]], axis=0).T
    for i in range(4):
        shift = (0 - flag[step * 4 + i] * amount[step * 4 + i]) & (N - 1)
        kx_index = jnp.full((32, N), row * 8 + step * 4 + i, jnp.int32)
        kz_index = lax.broadcasted_iota(jnp.int32, (32, N), 0) + col * 32
        ky_index = lax.broadcasted_iota(jnp.int32, (32, N), 1)
        kx, k1, kz, square, _ = modes(kx_index, kz_index, ky_index, drift)
        wave = (kx, k1, kz)
        coupling = 2.0 * shear[0] * kx / jnp.maximum(square, 1.0)
        damp = viscosity[0] * square
        for p in range(2):
            v = [pltpu.roll(velocity[c, p, i], shift, 1) for c in range(3)]
            for c in range(3):
                rate = result[c][p][32 * i:32 * i + 32] + coupling * wave[c] * v[1] - damp * v[c]
                if c == 0:
                    rate = rate - shear[0] * v[1]
                fresh = (-5.0 / 9.0) * pltpu.roll(accumulator[c, p, i], shift, 1) + time_step[0] * rate
                new_accumulator[c, p, i] = fresh
                new_velocity[c, p, i] = v[c] + (15.0 / 16.0) * fresh


def call(kernel, grid, limit, ins, outs, scratch=()):
    return pl.pallas_call(
        kernel,
        grid=grid,
        in_specs=ins,
        out_specs=[spec for spec, _ in outs],
        out_shape=[shape for _, shape in outs],
        scratch_shapes=list(scratch),
        compiler_params=pltpu.CompilerParams(vmem_limit_bytes=limit * MIB),
    )


def spec(shape, index):
    return pl.BlockSpec(shape, index)


def whole(array):
    rank = array.ndim
    return pl.BlockSpec(array.shape, lambda *_: (0,) * rank)


SMEM = pl.BlockSpec(memory_space=pltpu.SMEM)


def body(velocity, accumulator, remesh_flag, remesh_shift, viscosity, shear, clock, step):
    first, second, back, fore = [jnp.asarray(table) for table in tables()]
    shape = jax.ShapeDtypeStruct
    hbm = pl.BlockSpec(memory_space=pltpu.HBM)
    [hats] = pl.pallas_call(
        middle_kernel,
        in_specs=[hbm] * 2 + [SMEM] * 2 + [hbm] * 5,
        out_specs=[hbm],
        out_shape=[shape((4, BACK + 8, N), F32)],
        scratch_shapes=[
            pltpu.SMEM((8,), jnp.int32), pltpu.SMEM((8,), jnp.int32), pltpu.VMEM((4, BACK + 8, N), F32), pltpu.VMEM((2, BACK, 2 * N), BF16),
            pltpu.VMEM(velocity.shape, F32), pltpu.VMEM(first.shape, BF16), pltpu.VMEM(second.shape, BF16),
            pltpu.VMEM(back.shape, BF16), pltpu.VMEM(fore.shape, BF16),
            pltpu.VMEM((3, N, 2 * N), BF16), pltpu.VMEM((3, N, 2 * N), BF16), pltpu.VMEM((8, N), F32),
            pltpu.VMEM((3, 1024, 128), F32), pltpu.VMEM((3, 8, KX, 128), F32),
            pltpu.VMEM((4, 8, KX, 128), F32), pltpu.VMEM((4, 1024, 128), F32),
            pltpu.VMEM((8, 8, N), F32),
            pltpu.VMEM((3, N, 2 * N), F32), pltpu.VMEM((5, 2 * KX, 2 * N), F32), pltpu.VMEM((2, 4 * KX, 128), F32),
            pltpu.SemaphoreType.DMA((8,)), pltpu.SemaphoreType.DMA((8,)), pltpu.SemaphoreType.DMA((14,)),
        ],
        compiler_params=pltpu.CompilerParams(collective_id=0, has_side_effects=True, vmem_limit_bytes=60 * MIB),
    )(remesh_flag, remesh_shift, shear, clock, velocity, first, second, back, fore)
    state = spec((3, 2, 4, 32, N), lambda i: (0, 0, i, 0, 0))
    return call(
        post_kernel, (2,), 50,
        [SMEM] * 6 + [spec((4, BACK + 8, 128), lambda i: (0, 0, i)), state, state],
        [(state, shape(velocity.shape, F32)), (state, shape(velocity.shape, F32)),
         (spec((2, 8), lambda i: (0, 0)), shape((2, 8), F32))],
    )(remesh_flag, remesh_shift, viscosity, shear, clock, step, hats, velocity, accumulator)


def solution(mesh):
    state = P(None, None, "row", "col", None)
    return jax.shard_map(
        body,
        mesh=mesh,
        in_specs=(state, state, P("row"), P("row"), P(), P(), P(), P()),
        out_specs=(state, state, P(None, "row")),
        check_vma=False,
    )
```

```python
import numpy as np
import jax
import jax.numpy as jnp
from jax import lax
from jax.experimental import pallas as pl
from jax.experimental.pallas import tpu as pltpu
from jax.sharding import PartitionSpec as P

N = 256
ROWS = 11
COLS = (0, 1, 2, 5, 6, 7)
KX = 8 * ROWS
BACK = 2 * 192
F32 = jnp.float32
BF16 = jnp.bfloat16
MIB = 1024 * 1024


def halves(table):
    table = table.astype(np.float32)
    high = table.astype(jnp.bfloat16)
    low = (table - high.astype(np.float32)).astype(jnp.bfloat16)
    return np.stack([high, low])


def tables():
    index = np.arange(N)
    angle = (index[:, None] * index[None, :] % N) * (2.0 * np.pi / N)
    cos, sin = np.cos(angle) / 16.0, np.sin(angle) / 16.0
    first = np.block([[cos, -sin], [sin, cos]])
    second = np.block([[cos, sin], [-sin, cos]])
    place = np.arange(KX)
    order = 4 * (place % 22) + place // 22
    weights = np.where(order == 0, 1.0, 2.0)
    back_x = np.concatenate([cos[:, order] * weights, -sin[:, order] * weights], axis=1)
    fore_x = np.concatenate([cos[order], -sin[order]], axis=0)
    return halves(first), halves(second), halves(back_x), halves(fore_x)


def split(value):
    high = value.astype(BF16)
    return high, (value - high.astype(F32)).astype(BF16)


def dot3(left, right, dims=((1,), (0,))):
    def one(a, b):
        return lax.dot_general(a, b, (dims, ((), ())), preferred_element_type=F32)

    return one(left[0], right[0]) + one(left[1], right[0]) + one(left[0], right[1])


def swap_chunks(items, width):
    items = list(items)
    count = len(items)
    lane = lax.broadcasted_iota(jnp.int32, items[0].shape, items[0].ndim - 1) // width
    axis = items[0].ndim - 1
    step = count // 2
    while step:
        keep = (lane & step) == 0
        for i in range(count):
            if i & step == 0:
                a, b = items[i], items[i + step]
                items[i] = jnp.where(keep, a, pltpu.roll(b, step * width, axis))
                items[i + step] = jnp.where(keep, pltpu.roll(a, 128 - step * width, axis), b)
        step //= 2
    return items


def signed(index):
    return jnp.where(2 * index < N, index, index - N)


def modes(kx_index, kz_index, ky_index, drift):
    wave_x = kx_index.astype(F32)
    wave_z = signed(kz_index).astype(F32)
    wave_y = signed(ky_index).astype(F32) - drift * wave_x
    square = wave_x * wave_x + wave_y * wave_y + wave_z * wave_z
    mask = (3 * kx_index < N) & (3 * jnp.abs(signed(kz_index)) < N) & (3 * jnp.abs(signed(ky_index)) < N)
    return wave_x, wave_y, wave_z, square, mask


def remeshed_modes(kx_local, row, col, flag, amount, shear, clock, velocity):
    shift = (0 - flag[kx_local] * amount[kx_local]) & (N - 1)
    kx = jnp.full((32, N), row * 8 + kx_local, jnp.int32)
    kz = lax.broadcasted_iota(jnp.int32, (32, N), 0) + col * 32
    ky = lax.broadcasted_iota(jnp.int32, (32, N), 1)
    state = [[pltpu.roll(velocity[c, p, kx_local], shift, 1) for c in range(3)] for p in range(2)]
    return state, modes(kx, kz, ky, shear[0] * clock[0])


def project_modes(kx_local, state, waves, high, low):
    wave, square, mask = waves[:3], waves[3], waves[4]
    inverse = 1.0 / jnp.maximum(square, 1.0)
    rows = pl.ds(pl.multiple_of(kx_local * 32, 32), 32)
    for p in range(2):
        v = state[p]
        along = (wave[0] * v[0] + wave[1] * v[1] + wave[2] * v[2]) * inverse
        for slot, c in enumerate((0, 2, 1)):
            upper, lower = split(jnp.where(mask, v[c] - wave[c] * along, 0.0))
            high[slot, rows, p * N:(p + 1) * N] = upper
            low[slot, rows, p * N:(p + 1) * N] = lower


def add_spectra(kx_local, state, waves, sums):
    energy = jnp.zeros((32, N), F32)
    stress = jnp.zeros((32, N), F32)
    for v in state:
        energy += v[0] * v[0] + v[1] * v[1] + v[2] * v[2]
        stress += v[0] * v[1]

    def total(value):
        value = jnp.sum(value, axis=0, keepdims=True)
        return value[:, :128] + value[:, 128:]

    sums[pl.ds(kx_local, 1), :] = jnp.concatenate([total(stress), total(waves[3] * energy)], axis=1)


MESH = pl.DeviceIdType.MESH


def middle_kernel(flag_in, amount_in, shear, clock, velocity_in, first_in, second_in, back_in, fore_in,
                  hats_out, flag, amount, result, velocity, first, second, back, fore, high, low, sums,
                  send_b, recv_b, send_f, recv_f, recv_s, u, hats, data, out_sems, in_sems, load_sems):
    row, col = lax.axis_index("row"), lax.axis_index("col")
    me = row * 8 + col
    on = (row < ROWS) & (col != 3) & (col != 4)
    off = jnp.logical_not(on)

    def push(src, dst, sem, device):
        return pltpu.make_async_remote_copy(
            src_ref=src, dst_ref=dst, send_sem=out_sems.at[sem], recv_sem=in_sems.at[sem],
            device_id=device, device_id_type=MESH)

    def drain(blocks, sem):
        ref = recv_f.at[0, pl.ds(0, 8 * blocks)]
        pltpu.make_async_copy(ref, ref, sem).wait()

    to_cols = [lax.rem(col + j, 8) for j in range(8)]
    spots = [lax.rem(col + j, 6) for j in range(6)]
    on_cols = [spot + 2 * (spot // 3) for spot in spots]
    barrier = pltpu.get_barrier_semaphore()

    def greet(i, carry):
        to_row = lax.rem(row + i, 16)
        for j in range(8):
            @pl.when((i > 0) | (j > 0))
            def _():
                pl.semaphore_signal(barrier, inc=1, device_id={"row": to_row, "col": to_cols[j]}, device_id_type=MESH)
        return carry

    loads = [pltpu.make_async_copy(velocity_in.at[:, :, kx], velocity.at[:, :, kx], load_sems.at[kx]) for kx in range(8)]
    for i, (source, target) in enumerate(((first_in, first), (second_in, second), (back_in, back), (fore_in, fore))):
        loads.append(pltpu.make_async_copy(source, target, load_sems.at[8 + i]))
    for i, (source, target) in enumerate(((flag_in, flag), (amount_in, amount))):
        loads.append(pltpu.make_async_copy(source, target, load_sems.at[12 + i]))
    for load in loads[12:] + loads[:12]:
        load.start()
    lax.fori_loop(0, 16, greet, 0)

    def prepare(kx, carry):
        pltpu.make_async_copy(velocity_in.at[:, :, kx], velocity.at[:, :, kx], load_sems.at[kx]).wait()

        @pl.when(on)
        def _():
            project_modes(kx, *remeshed_modes(kx, row, col, flag, amount, shear, clock, velocity), high, low)

        return carry

    for load in loads[12:]:
        load.wait()
    lax.fori_loop(0, 8, prepare, 0, unroll=2)
    for load in loads[8:12]:
        load.wait()
    pl.semaphore_wait(barrier, 127)
    @pl.when(on)
    def _():
        def y_back(f, carry):
            result = dot3((first[0], first[1]), (high[f], low[f]), ((1,), (1,)))
            for h in range(2):
                for plane in range(2):
                    for p in range(2):
                        start = p * N + plane * 128
                        send_b[f, pl.ds((h * 2 + plane) * 2 + p, 128, stride=8), :] = (
                            result[start:start + 128, 128 * h:128 * h + 128])

            def send(i, carry):
                to_row = lax.rem(row + i, 16)
                for j in range(8):
                    @pl.when((i > 0) | (j > 0))
                    def _():
                        push(send_b.at[f, pl.ds(to_row * 64 + to_cols[j] * 8, 8)],
                             recv_b.at[f, col, pl.ds(row * 8, 8)], f, {"row": to_row, "col": to_cols[j]}).start()
                return carry

            lax.fori_loop(0, 16, send, 0)
            recv_b[f, col, pl.ds(row * 8, 8), :] = send_b[f, pl.ds(me * 8, 8), :]
            return carry

        lax.fori_loop(0, 3, y_back, 0)

    def spectra_of(kx, carry):
        add_spectra(kx, *remeshed_modes(kx, row, col, flag, amount, shear, clock, velocity), sums)
        return carry

    lax.fori_loop(0, 8, spectra_of, 0)
    for i in range(1, 8):
        push(sums, recv_s.at[col], 7, {"col": (col + i) % 8}).start()

    def to_grid(f):
        @pl.when(on)
        def _():
            drain(65, in_sems.at[f])

        @pl.when(off)
        def _():
            drain(66, in_sems.at[f])

        for g in range(2):
            blocks = [recv_b[f, c] if c in COLS else jnp.zeros((KX, 128), F32) for c in range(4 * g, 4 * g + 4)]
            moved = swap_chunks(blocks, 32)
            for i in range(4):
                data[g, KX * i:KX * i + KX, :] = moved[i]
        modes_in = jnp.concatenate(
            [jnp.concatenate([data[g, pl.ds(plane * 2 + p, KX, stride=4), :] for p in range(2) for g in range(2)], axis=1)
             for plane in range(2)], axis=0)
        lines = dot3(split(modes_in), (second[0], second[1]))
        for plane in range(2):
            both = jnp.concatenate([lines[KX * plane:KX * plane + KX, p * N:p * N + N] for p in range(2)], axis=0)
            u[f, :, plane * N:plane * N + N] = dot3((back[0], back[1]), split(both))

    def to_modes(t):
        a = jnp.where((t == 0) | (t == 2), 0, jnp.where(t == 4, 2, 1))
        b = jnp.where(t < 2, 1, 2)
        weight = jnp.where((t == 1) | (t == 4), 1.0, 0.0)
        planes = []
        for plane in range(2):
            lanes = slice(plane * N, plane * N + N)
            field = u[a, :, lanes] * u[b, :, lanes] - weight * (u[0, :, lanes] * u[0, :, lanes])
            hat = dot3((fore[0], fore[1]), split(field))
            planes.append(jnp.concatenate([hat[:KX], hat[KX:]], axis=1))
        hats[t] = dot3(split(jnp.concatenate(planes, axis=0)), (first[0], first[1]))

    place = lax.broadcasted_iota(jnp.int32, (KX, N), 0)
    group = (place >= 22).astype(jnp.int32) + (place >= 44).astype(jnp.int32) + (place >= 66).astype(jnp.int32)
    kx_index = 4 * (place - 22 * group) + group
    kz_index = lax.broadcasted_iota(jnp.int32, (KX, N), 1)
    kx = kx_index.astype(F32)
    kz = signed(kz_index).astype(F32)
    origin = (kx_index == 0) & (kz_index == 0)

    def field_out(g, formula):
        for plane in range(2):
            for p in range(2):
                value = formula(lambda t: hats[t, plane * KX:plane * KX + KX, p * N:p * N + N])
                for half in range(2):
                    data[half, pl.ds(plane * 2 + p, KX, stride=4), :] = value[:, 128 * half:128 * half + 128]
        for half in range(2):
            moved = swap_chunks([data[half, KX * i:KX * i + KX, :] for i in range(4)], 32)
            for i in range(4):
                if 4 * half + i in COLS:
                    send_f[g, 4 * half + i] = moved[i]

        def send(i, carry):
            to_row = lax.rem(row + i, ROWS)
            for to_col in on_cols:
                @pl.when((to_row != row) | (to_col != col))
                def _():
                    push(send_f.at[g, to_col, pl.ds(to_row * 8, 8)], recv_f.at[g, pl.ds(me * 8, 8)], 3 + g,
                         {"row": to_row, "col": to_col}).start()
            return carry

        lax.fori_loop(0, ROWS, send, 0)

        @pl.when(on)
        def _():
            recv_f[g, pl.ds(me * 8, 8), :] = send_f[g, col, pl.ds(row * 8, 8), :]

    def step_of(step, carry):
        backward = (step == 0) | (step == 1) | (step == 4)

        @pl.when(backward)
        def _():
            to_grid(jnp.where(step == 4, 2, jnp.minimum(step, 2)))

        @pl.when(jnp.logical_not(backward))
        def _():
            to_modes(jnp.where(step < 4, step - 2, step - 3))

        @pl.when(step == 3)
        def _():
            field_out(0, lambda t: (kz * kz - kx * kx) * t(0) - kx * kz * t(1))

        @pl.when(step == 6)
        def _():
            field_out(1, lambda t: jnp.where(origin, t(2), kx * t(2) + kz * t(3)))
            field_out(2, lambda t: jnp.where(origin, t(3), kz * t(2) - kx * t(3)))

        @pl.when(step == 7)
        def _():
            field_out(3, lambda t: 2.0 * kx * kz * t(0) + kz * kz * t(1) - (kx * kx + kz * kz) * t(4))

        return carry

    lax.fori_loop(0, 8, step_of, 0)

    drain_sums = recv_s.at[pl.ds(0, 7)]
    pltpu.make_async_copy(drain_sums, drain_sums, in_sems.at[7]).wait()
    recv_s[col] = sums[...]
    total = recv_s[0]
    for i in range(1, 8):
        total = total + recv_s[i]
    for g in range(4):
        result[g, BACK:BACK + 8, :] = total

    @pl.when(on)
    def _():
        def y_fore(g, carry):
            drain(127, in_sems.at[3 + g])
            both = jnp.concatenate(
                [jnp.concatenate([recv_f[g, pl.ds((h * 2 + plane) * 2 + p, 128, stride=8), :] for h in range(2)], axis=1)
                 for p in range(2) for plane in range(2)], axis=0)
            table = [jnp.concatenate([second[i, start:start + 96] for start in (0, 160, 256, 416)], axis=0) for i in range(2)]
            result[g, :BACK, :] = dot3(table, split(both))
            pltpu.make_async_copy(result.at[g], hats_out.at[g], load_sems.at[g]).start()
            return carry

        lax.fori_loop(0, 4, y_fore, 0)

    @pl.when(off)
    def _():
        for g in range(4):
            result[g, :BACK, :] = jnp.zeros((BACK, N), F32)
            pltpu.make_async_copy(result.at[g], hats_out.at[g], load_sems.at[g]).start()

    for g in range(4):
        pltpu.make_async_copy(result.at[g], hats_out.at[g], load_sems.at[g]).wait()

    pltpu.make_async_copy(drain_sums, drain_sums, out_sems.at[7]).wait()

    @pl.when(on)
    def _():
        for f in range(3):
            drain(127, out_sems.at[f])
        for g in range(4):
            drain(65, out_sems.at[3 + g])

    @pl.when(off)
    def _():
        for g in range(4):
            drain(66, out_sems.at[3 + g])


def post_kernel(flag, amount, viscosity, shear, clock, time_step, block, velocity, accumulator,
                new_velocity, new_accumulator, spectra):
    step = pl.program_id(0)
    row, col = lax.axis_index("row"), lax.axis_index("col")
    drift = shear[0] * clock[0]

    diagonal = lax.broadcasted_iota(jnp.int32, (8, 8), 0) == lax.broadcasted_iota(jnp.int32, (8, 8), 1)
    factor = jnp.where(step == 0, 1.0, 2.0 * viscosity[0]) / (N * N)
    value = jnp.sum(block[0, BACK:BACK + 8, :], axis=1, keepdims=True) * factor
    spectra[pl.ds(step, 1), :] = jnp.sum(jnp.where(diagonal, value, 0.0), axis=0, keepdims=True)

    hats = [(block[g, :192], block[g, 192:384]) for g in (1, 3, 0, 2)]
    lane = lax.broadcasted_iota(jnp.int32, (192, 128), 1)
    kx_index = lane // 32 + (row * 8 + step * 4)
    kz_index = lane % 32 + col * 32
    place = lax.broadcasted_iota(jnp.int32, (192, 128), 0)
    ky_index = jnp.where(place < 96, place, place + 64)
    kx, k1, kz, square, mask = modes(kx_index, kz_index, ky_index, drift)
    flat = kx * kx + kz * kz
    origin = flat == 0.0
    over_square = 1.0 / jnp.maximum(square, 1.0)
    over_flat = 1.0 / jnp.maximum(flat, 1.0)
    result = [[None, None] for _ in range(3)]
    for p in range(2):
        sign = -1.0 if p == 0 else 1.0
        x, q, r, s = [sign * hats[g][1 - p] for g in range(4)]
        v = ((k1 * k1 - flat) * x + k1 * q) * over_square
        w = 0.0 - (r + k1 * s)
        part = [
            jnp.where(origin, 0.0 - k1 * x, (kz * w - kx * k1 * v) * over_flat),
            jnp.where(origin, 0.0, v),
            jnp.where(origin, 0.0 - k1 * s, (0.0 - kx * w - kz * k1 * v) * over_flat),
        ]
        for c in range(3):
            kept = jnp.where(mask, part[c], 0.0)
            result[c][p] = jnp.concatenate([kept[:96], jnp.zeros((64, 128), F32), kept[96:]], axis=0).T
    for i in range(4):
        shift = (0 - flag[step * 4 + i] * amount[step * 4 + i]) & (N - 1)
        kx_index = jnp.full((32, N), row * 8 + step * 4 + i, jnp.int32)
        kz_index = lax.broadcasted_iota(jnp.int32, (32, N), 0) + col * 32
        ky_index = lax.broadcasted_iota(jnp.int32, (32, N), 1)
        kx, k1, kz, square, _ = modes(kx_index, kz_index, ky_index, drift)
        wave = (kx, k1, kz)
        coupling = 2.0 * shear[0] * kx / jnp.maximum(square, 1.0)
        damp = viscosity[0] * square
        for p in range(2):
            v = [pltpu.roll(velocity[c, p, i], shift, 1) for c in range(3)]
            for c in range(3):
                rate = result[c][p][32 * i:32 * i + 32] + coupling * wave[c] * v[1] - damp * v[c]
                if c == 0:
                    rate = rate - shear[0] * v[1]
                fresh = (-5.0 / 9.0) * pltpu.roll(accumulator[c, p, i], shift, 1) + time_step[0] * rate
                new_accumulator[c, p, i] = fresh
                new_velocity[c, p, i] = v[c] + (15.0 / 16.0) * fresh


def call(kernel, grid, limit, ins, outs, scratch=()):
    return pl.pallas_call(
        kernel,
        grid=grid,
        in_specs=ins,
        out_specs=[spec for spec, _ in outs],
        out_shape=[shape for _, shape in outs],
        scratch_shapes=list(scratch),
        compiler_params=pltpu.CompilerParams(vmem_limit_bytes=limit * MIB),
    )


def spec(shape, index):
    return pl.BlockSpec(shape, index)


def whole(array):
    rank = array.ndim
    return pl.BlockSpec(array.shape, lambda *_: (0,) * rank)


SMEM = pl.BlockSpec(memory_space=pltpu.SMEM)


def body(velocity, accumulator, remesh_flag, remesh_shift, viscosity, shear, clock, step):
    first, second, back, fore = [jnp.asarray(table) for table in tables()]
    shape = jax.ShapeDtypeStruct
    hbm = pl.BlockSpec(memory_space=pltpu.HBM)
    [hats] = pl.pallas_call(
        middle_kernel,
        in_specs=[hbm] * 2 + [SMEM] * 2 + [hbm] * 5,
        out_specs=[hbm],
        out_shape=[shape((4, BACK + 8, N), F32)],
        scratch_shapes=[
            pltpu.SMEM((8,), jnp.int32), pltpu.SMEM((8,), jnp.int32), pltpu.VMEM((4, BACK + 8, N), F32),
            pltpu.VMEM(velocity.shape, F32), pltpu.VMEM(first.shape, BF16), pltpu.VMEM(second.shape, BF16),
            pltpu.VMEM(back.shape, BF16), pltpu.VMEM(fore.shape, BF16),
            pltpu.VMEM((3, N, 2 * N), BF16), pltpu.VMEM((3, N, 2 * N), BF16), pltpu.VMEM((8, N), F32),
            pltpu.VMEM((3, 1024, 128), F32), pltpu.VMEM((3, 8, KX, 128), F32),
            pltpu.VMEM((4, 8, KX, 128), F32), pltpu.VMEM((4, 1024, 128), F32),
            pltpu.VMEM((8, 8, N), F32),
            pltpu.VMEM((3, N, 2 * N), F32), pltpu.VMEM((5, 2 * KX, 2 * N), F32), pltpu.VMEM((2, 4 * KX, 128), F32),
            pltpu.SemaphoreType.DMA((8,)), pltpu.SemaphoreType.DMA((8,)), pltpu.SemaphoreType.DMA((14,)),
        ],
        compiler_params=pltpu.CompilerParams(collective_id=0, has_side_effects=True, vmem_limit_bytes=60 * MIB),
    )(remesh_flag, remesh_shift, shear, clock, velocity, first, second, back, fore)
    state = spec((3, 2, 4, 32, N), lambda i: (0, 0, i, 0, 0))
    return call(
        post_kernel, (2,), 50,
        [SMEM] * 6 + [spec((4, BACK + 8, 128), lambda i: (0, 0, i)), state, state],
        [(state, shape(velocity.shape, F32)), (state, shape(velocity.shape, F32)),
         (spec((2, 8), lambda i: (0, 0)), shape((2, 8), F32))],
    )(remesh_flag, remesh_shift, viscosity, shear, clock, step, hats, velocity, accumulator)


def solution(mesh):
    state = P(None, None, "row", "col", None)
    return jax.shard_map(
        body,
        mesh=mesh,
        in_specs=(state, state, P("row"), P("row"), P(), P(), P(), P()),
        out_specs=(state, state, P(None, "row")),
        check_vma=False,
    )
```
